32 devices in a mesh: pix: 8 (over y, x, core), row: 4 (over z).
Axes of the slice: x: 2, y: 2, z: 4, core: 2. Of those that a mesh axis runs over, the one named last changes fastest.
Arguments:
- band_images: bfloat16 [256, 128, 512], P('pix', 'row'), may hold values from -6 to 6
- pivots: int32 [2, 32], replicated, may hold values from 0 to 65535, as said below
Outputs:
- residual: bfloat16 [512, 128, 256], P(('pix', 'row'))
- coefficients: bfloat16 [64, 512, 128], P(None, ('pix', 'row'))
The draws below stay inside these ranges and needn't reach their ends.
Inputs may be any that keep to these rules, and one draw needn't show every extreme that they name: All 64 pivots lie in different columns, and every group of 32 lines starting at a multiple of 32 holds at least one pivot.
All inputs are finite; a program needn't handle non-finite values.
Results may differ from the reference program's by a relative error of at most 0.001.
Values may be sent and summed in bfloat16 or wider, within the bound.
No kernel may reach another device: no remote copies, remote signals or barrier semaphores. Data moves between devices by JAX's collectives and lax.ppermute only.
A program may use at most 192 MiB of HBM per device.

```python
import jax
import jax.numpy as jnp
from jax import lax

B = 256
NPIV = 32
LINE_DEV = 32
LINES = 128
COLS = 512
N_PIX = 8


def draw_pivots(key, part):
    key_cols, key_group, key_first, key_inner = jax.random.split(jax.random.fold_in(key, 11), 4)
    total = 2 * NPIV
    groups = LINES // LINE_DEV
    columns = jax.random.permutation(key_cols, COLS)[:total].astype(jnp.int32)
    chosen = jax.random.randint(key_group, (total,), 0, groups).astype(jnp.int32)
    chosen = chosen.at[:groups].set(jax.random.permutation(key_first, groups).astype(jnp.int32))
    inner = jax.random.randint(key_inner, (total,), 0, LINE_DEV).astype(jnp.int32)
    line_index = chosen * LINE_DEV + inner
    return (line_index * COLS + columns).reshape(2, NPIV).astype(jnp.int32)


def block_levels(stream_key, shape, cuts, low, largest):
    def one(position, shards_of):
        heights = jax.random.uniform(jax.random.fold_in(jax.random.fold_in(stream_key, 6), position), (shards_of,), jnp.float32, low / len(cuts), largest / len(cuts))
        return jnp.repeat(jnp.exp(heights), shape[position] // shards_of).reshape((-1,) + (1,) * (len(shape) - position - 1))

    level = one(*cuts[0])
    for cut in cuts[1:]:
        level = level * one(*cut)
    return level


def centred(own_key, dims, spread, reach, cuts=(), kind=jnp.bfloat16):
    drawn = jax.random.normal(own_key, dims, jnp.float32) * spread
    if len(cuts) > 0:
        drawn = block_levels(own_key, dims, cuts, -0.22, 0.18) * drawn
    return jnp.clip(drawn, min=-reach, max=reach).astype(kind)


def setup_inputs(seed: int = 0) -> dict:
    key_of = jax.random.split(jax.random.key(seed), 3)
    return {
        "band_images": centred(key_of[0], (B, LINES, COLS), 1.0, 6.0, ((0, 8), (1, 4))),
        "pivots": draw_pivots(jax.random.fold_in(key_of[2], 71), 0),
    }


highest = lax.Precision.HIGHEST

def orthonormal(spectra):
    gram = jnp.dot(spectra, spectra.T, precision=highest)
    factor = jnp.linalg.cholesky(gram)
    return jax.scipy.linalg.solve_triangular(factor, spectra, lower=True)

def project(block, basis):
    count = basis.shape[0] // 2
    first = basis[:count]
    second = basis[count:]
    coef_one = jnp.einsum('clb,kb->kcl', block, first, precision=highest)
    remain = block - jnp.einsum('kcl,kb->clb', coef_one, first, precision=highest)
    coef_two = jnp.einsum('clb,kb->kcl', remain, second, precision=highest)
    remain = remain - jnp.einsum('kcl,kb->clb', coef_two, second, precision=highest)
    return (remain.astype(jnp.bfloat16), jnp.concatenate([coef_one, coef_two], axis=0).astype(jnp.bfloat16))

def reference(band_images, pivots):
    flat_images = band_images.reshape(B, LINES * COLS)
    spectra = jnp.take(flat_images, pivots.reshape(-1), axis=1).T.astype(jnp.float32)
    basis = orthonormal(spectra)
    width = COLS // N_PIX

    def one_group(group):
        start = (group * width).astype(jnp.int32)
        piece = lax.dynamic_slice_in_dim(band_images, start, width, 2)
        block = piece.transpose(2, 1, 0).astype(jnp.float32)
        return project(block, basis)
    remains, coefs = lax.map(one_group, jnp.arange(N_PIX, dtype=jnp.int32))
    residual = remains.reshape(COLS, LINES, B)
    coefficients = coefs.transpose(1, 0, 2, 3).reshape(2 * NPIV, COLS, LINES)
    return (residual, coefficients)
```

```python
import jax
import jax.numpy as jnp
from jax import lax
from jax.experimental import pallas as pl
from jax.experimental.pallas import tpu as pltpu
from jax.sharding import PartitionSpec as P

highest = lax.Precision.HIGHEST
f32 = jnp.float32
bf16 = jnp.bfloat16
LANES = 128
SUBLANES = 8
AXES = ("pix", "row")


def contract_last(a, b):
    return lax.dot_general(a, b, (((1,), (1,)), ((), ())), preferred_element_type=f32)


def pack(band_images, column, inner, part_count):
    band_dev, line_dev, cols = band_images.shape
    rows = band_dev * line_dev
    taken = LANES // band_dev
    groups = line_dev // taken
    pivot_count = column.shape[0]
    half = band_dev // 2
    col_step = 2 * LANES

    def kernel(x_ref, col_ref, in_ref, out_ref, spec_ref, wide_ref, rows_ref):
        for c in range(cols // LANES):
            wide_ref[c] = (
                x_ref[:, :, c * LANES : (c + 1) * LANES].astype(f32).reshape(rows, LANES)
            )
        for c in range(cols // LANES):
            for g in range(groups):
                for t in range(taken):
                    line = t * groups + g
                    start = (g * taken + t) * band_dev
                    part = wide_ref[c, pl.ds(line, band_dev, stride=line_dev), :]
                    rows_ref[start : start + band_dev, c * LANES : (c + 1) * LANES] = part.astype(bf16)
        picked = jnp.zeros((pivot_count, rows), f32)
        eye = (
            lax.broadcasted_iota(jnp.int32, (col_step, col_step), 0)
            == lax.broadcasted_iota(jnp.int32, (col_step, col_step), 1)
        ).astype(f32).astype(bf16)
        for c in range(cols // col_step):
            block = rows_ref[:, c * col_step : (c + 1) * col_step]
            hot = (
                lax.broadcasted_iota(jnp.int32, (pivot_count, col_step), 1) + c * col_step
                == col_ref[...]
            ).astype(f32).astype(bf16)
            both = contract_last(jnp.concatenate([eye, hot], axis=0), block)
            out_ref[c * col_step : (c + 1) * col_step, :] = both[:col_step].astype(bf16)
            picked = picked + both[col_step:]
        lane = lax.broadcasted_iota(jnp.int32, (pivot_count, rows), 1)
        piece = lane // band_dev
        line = (piece % taken) * groups + piece // taken
        picked = jnp.where(line == in_ref[...], picked, 0.0).astype(bf16)
        fold = (
            lax.broadcasted_iota(jnp.int32, (band_dev, rows), 1) % band_dev
            == lax.broadcasted_iota(jnp.int32, (band_dev, rows), 0)
        ).astype(f32).astype(bf16)
        found = contract_last(fold, picked)
        found = jnp.concatenate([found[:half], found[half:]], axis=1).astype(bf16)
        spec_ref[...] = jnp.broadcast_to(found[None], spec_ref.shape)

    return pl.pallas_call(
        kernel,
        out_shape=(
            jax.ShapeDtypeStruct((cols, rows), bf16),
            jax.ShapeDtypeStruct((part_count, half, 2 * pivot_count), bf16),
        ),
        scratch_shapes=[
            pltpu.VMEM((cols // LANES, rows, LANES), f32),
            pltpu.VMEM((rows, cols), bf16),
        ],
        name="pack",
    )(band_images, column, inner)


def finish(arrived, keep, gains, pix_count, row_count, band_dev, line_dev):
    sources, narrow, rows = arrived.shape
    taken = LANES // band_dev
    groups = line_dev // taken
    lines = row_count * line_dev
    bands = pix_count * band_dev
    kept = gains.shape[0] // 2
    width = 4
    joined = bands // LANES

    def swap(low, high, shift, mask):
        return (
            jnp.where(mask, low, pltpu.roll(high, shift, 1)),
            jnp.where(mask, pltpu.roll(low, LANES - shift, 1), high),
        )

    def kernel(a_ref, keep_ref, gain_ref, res_ref, coef_ref, wide_ref, x_ref, hold_ref):
        for s in range(sources):
            for g in range(rows // LANES):
                wide_ref[s * (rows // LANES) + g] = a_ref[s, :, g * LANES : (g + 1) * LANES].astype(f32)
        flat = wide_ref.reshape(sources * (rows // LANES) * narrow, LANES)
        lane = lax.broadcasted_iota(jnp.int32, (SUBLANES, LANES), 1)
        for c in range(narrow):
            for r in range(row_count):
                for j in range(joined):
                    v = []
                    for i in range(taken):
                        source = (j * taken + i) * row_count + r
                        v.append(flat[pl.ds(source * (rows // LANES) * narrow + c, groups, stride=narrow), :])
                    step = taken // 2
                    while step >= 1:
                        shift = step * band_dev
                        mask = (lane // shift) % 2 == 0
                        w = list(v)
                        for i in range(taken):
                            if (i // step) % 2 == 0:
                                w[i], w[i + step] = swap(v[i], v[i + step], shift, mask)
                        v = w
                        step //= 2
                    row = c * lines + r * line_dev
                    x_ref[row : row + line_dev, j * LANES : (j + 1) * LANES] = (
                        jnp.concatenate(v, axis=0).astype(bf16)
                    )
        for s in range(0, narrow, width):
            pixels = x_ref[s * lines : (s + width) * lines, :]
            both = jnp.dot(pixels, keep_ref[:bands], preferred_element_type=f32)
            both = both + jnp.dot(pixels, keep_ref[bands:], preferred_element_type=f32)
            res_ref[s : s + width] = both.astype(bf16).reshape(width, lines, bands)
            found = contract_last(gain_ref[...], pixels)
            found = found[:kept] + found[kept:]
            for i in range(width):
                hold_ref[:, s + i, :] = found[:, i * lines : (i + 1) * lines]
        coef_ref[...] = hold_ref[...].astype(bf16)

    return pl.pallas_call(
        kernel,
        out_shape=(
            jax.ShapeDtypeStruct((narrow, lines, bands), bf16),
            jax.ShapeDtypeStruct((kept, narrow, lines), bf16),
        ),
        scratch_shapes=[
            pltpu.VMEM((sources * (rows // LANES), narrow, LANES), f32),
            pltpu.VMEM((narrow * lines, bands), bf16),
            pltpu.VMEM((kept, narrow, lines), f32),
        ],
        name="finish",
    )(arrived, keep, gains)


def split(a):
    high = lax.reduce_precision(a, 8, 7)
    return jnp.concatenate([high, a - high], axis=0).astype(bf16)


def orthonormal(spectra):
    gram = jnp.dot(spectra, spectra.T, precision=highest)
    factor = jnp.linalg.cholesky(gram)
    return jax.scipy.linalg.solve_triangular(factor, spectra, lower=True)


def operators(basis):
    count = basis.shape[0] // 2
    first = basis[:count]
    second = basis[count:]
    cross = jnp.dot(second, first.T, precision=highest)
    second_gain = second - jnp.dot(cross, first, precision=highest)
    gains = jnp.concatenate([first, second_gain], axis=0)
    keep = jnp.eye(basis.shape[1], dtype=f32) - jnp.dot(gains.T, basis, precision=highest)
    return keep, gains


def project(block, basis):
    count = basis.shape[0] // 2
    first = basis[:count]
    second = basis[count:]
    coef_one = jnp.einsum("clb,kb->kcl", block, first, precision=highest)
    remain = block - jnp.einsum("kcl,kb->clb", coef_one, first, precision=highest)
    coef_two = jnp.einsum("clb,kb->kcl", remain, second, precision=highest)
    remain = remain - jnp.einsum("kcl,kb->clb", coef_two, second, precision=highest)
    return (
        remain.astype(bf16),
        jnp.concatenate([coef_one, coef_two], axis=0).astype(bf16),
    )


def plain(band_images, line_index, column, pix_count, row_count, narrow):
    band_dev, line_dev, cols_all = band_images.shape
    offset = line_index - lax.axis_index("row") * line_dev
    inside = (offset >= 0) & (offset < line_dev)
    position = jnp.clip(offset, 0, line_dev - 1) * cols_all + column
    picked = jnp.take(band_images.reshape(band_dev, line_dev * cols_all), position, axis=1)
    picked = jnp.where(inside[None, :], picked, jnp.zeros_like(picked))
    stacked = lax.all_gather(picked, "pix", axis=0, tiled=True)
    spectra = lax.psum(stacked.astype(f32).astype(bf16), "row").astype(f32)
    basis = orthonormal(spectra.T)
    shaped = band_images.reshape(band_dev, line_dev, pix_count, row_count, narrow)
    arrived = lax.all_to_all(
        lax.all_to_all(shaped, "pix", split_axis=2, concat_axis=0, tiled=True),
        "row",
        split_axis=3,
        concat_axis=1,
        tiled=True,
    )
    block = (
        arrived.reshape(arrived.shape[0], arrived.shape[1], narrow)
        .transpose(2, 1, 0)
        .astype(f32)
    )
    return project(block, basis)


def shards(band_images, pivots):
    band_dev, line_dev, cols_all = band_images.shape
    pix_count = lax.axis_size("pix")
    row_count = lax.axis_size("row")
    part_count = pix_count * row_count
    narrow = cols_all // part_count
    flat_pivots = pivots.reshape(-1)
    pivot_count = flat_pivots.shape[0]
    line_index = flat_pivots // cols_all
    column = flat_pivots % cols_all
    lines = row_count * line_dev
    bands = pix_count * band_dev
    taken = LANES // band_dev
    fits = (
        taken * band_dev == LANES
        and taken in (1, 2, 4, 8)
        and line_dev == SUBLANES * taken
        and narrow % 16 == 0
        and cols_all % (2 * LANES) == 0
        and lines == LANES
        and bands % LANES == 0
        and 2 * pivot_count == LANES
    )
    if not fits:
        return plain(band_images, line_index, column, pix_count, row_count, narrow)
    inner = line_index - lax.axis_index("row") * line_dev
    packed, picked = pack(band_images, column[:, None], inner[:, None], part_count)
    spectra = lax.all_to_all(picked, AXES, 0, 0, tiled=True)
    spectra = spectra.astype(f32).reshape(pix_count, row_count, band_dev // 2, 2, pivot_count).sum(1)
    spectra = spectra.transpose(3, 0, 2, 1).reshape(pivot_count, bands)
    basis = orthonormal(spectra)
    keep, gains = operators(basis)
    arrived = lax.all_to_all(packed.reshape(part_count, narrow, line_dev * band_dev), AXES, 0, 0, tiled=True)
    return finish(arrived, split(keep), split(gains), pix_count, row_count, band_dev, line_dev)


def solution(mesh):
    placed = (P("pix", "row", None), P())
    return jax.shard_map(
        shards,
        mesh=mesh,
        in_specs=placed,
        out_specs=(P(AXES, None, None), P(None, AXES, None)),
        check_vma=False,
    )
```

```python
import jax
import jax.numpy as jnp
from jax import lax
from jax.experimental import pallas as pl
from jax.experimental.pallas import tpu as pltpu
from jax.sharding import PartitionSpec as P


highest = lax.Precision.HIGHEST
f32 = jnp.float32
bf16 = jnp.bfloat16
LANES = 128
SUBLANES = 8
AXES = ("pix", "row")


def contract_last(a, b):
    return lax.dot_general(a, b, (((1,), (1,)), ((), ())), preferred_element_type=f32)


def pick(band_images, pivots, row_index):
    band_dev, line_dev, cols = band_images.shape
    rows = band_dev * line_dev
    panels, panel = pivots.shape
    pivot_count = panels * panel
    shift = cols.bit_length() - 1

    def kernel(row_ref, x_ref, piv_ref, spec_ref):
        flat = jnp.concatenate([piv_ref[i : i + 1, :] for i in range(panels)], axis=1)
        column = flat & (cols - 1)
        inner = (flat >> shift) - row_ref[0] * line_dev
        hot = (
            lax.broadcasted_iota(jnp.int32, (cols, pivot_count), 0) == column
        ).astype(f32).astype(bf16)
        found = jnp.dot(x_ref[...].reshape(rows, cols), hot, preferred_element_type=f32)
        line = lax.broadcasted_iota(jnp.int32, (line_dev, pivot_count), 0)
        found = jnp.where((line == inner)[None], found.reshape(band_dev, line_dev, pivot_count), 0.0)
        spec_ref[...] = jnp.sum(found, axis=1).astype(bf16)

    return pl.pallas_call(
        kernel,
        out_shape=jax.ShapeDtypeStruct((band_dev, pivot_count), bf16),
        in_specs=[
            pl.BlockSpec(memory_space=pltpu.SMEM),
            pl.BlockSpec(memory_space=pltpu.VMEM),
            pl.BlockSpec(memory_space=pltpu.VMEM),
        ],
        name="pick",
    )(row_index, band_images, pivots)


def pack(band_images):
    band_dev, line_dev, cols = band_images.shape
    rows = band_dev * line_dev
    taken = LANES // band_dev
    groups = line_dev // taken
    col_step = 2 * LANES

    def kernel(x_ref, out_ref, wide_ref, rows_ref):
        eye = (
            lax.broadcasted_iota(jnp.int32, (col_step, col_step), 0)
            == lax.broadcasted_iota(jnp.int32, (col_step, col_step), 1)
        ).astype(f32).astype(bf16)
        for c in range(cols // LANES):
            lanes = slice(c * LANES, (c + 1) * LANES)
            wide_ref[c] = x_ref[:, :, lanes].astype(f32).reshape(rows, LANES)
            for g in range(groups):
                for t in range(taken):
                    line = t * groups + g
                    start = (g * taken + t) * band_dev
                    part = wide_ref[c, pl.ds(line, band_dev, stride=line_dev), :]
                    rows_ref[start : start + band_dev, lanes] = part.astype(bf16)
            if c % 2 == 1:
                both = slice((c - 1) * LANES, (c + 1) * LANES)
                out_ref[both, :] = contract_last(eye, rows_ref[:, both]).astype(bf16)

    return pl.pallas_call(
        kernel,
        out_shape=jax.ShapeDtypeStruct((cols, rows), bf16),
        scratch_shapes=[
            pltpu.VMEM((cols // LANES, rows, LANES), f32),
            pltpu.VMEM((rows, cols), bf16),
        ],
        name="pack",
    )(band_images)


def finish(arrived, keep, gains, pix_count, row_count, band_dev, line_dev):
    sources, narrow, rows = arrived.shape
    taken = LANES // band_dev
    groups = line_dev // taken
    lines = row_count * line_dev
    bands = pix_count * band_dev
    kept = gains.shape[0] // 2
    width = 4
    joined = bands // LANES

    def swap(low, high, shift, mask):
        return (
            jnp.where(mask, low, pltpu.roll(high, shift, 1)),
            jnp.where(mask, pltpu.roll(low, LANES - shift, 1), high),
        )

    def kernel(a_ref, keep_ref, gain_ref, res_ref, coef_ref, wide_ref, x_ref, hold_ref):
        for s in range(sources):
            for g in range(rows // LANES):
                wide_ref[s * (rows // LANES) + g] = a_ref[s, :, g * LANES : (g + 1) * LANES].astype(f32)
        flat = wide_ref.reshape(sources * (rows // LANES) * narrow, LANES)
        lane = lax.broadcasted_iota(jnp.int32, (SUBLANES, LANES), 1)
        for c in range(narrow):
            for r in range(row_count):
                for j in range(joined):
                    v = []
                    for i in range(taken):
                        source = (j * taken + i) * row_count + r
                        v.append(flat[pl.ds(source * (rows // LANES) * narrow + c, groups, stride=narrow), :])
                    step = taken // 2
                    while step >= 1:
                        shift = step * band_dev
                        mask = (lane // shift) % 2 == 0
                        w = list(v)
                        for i in range(taken):
                            if (i // step) % 2 == 0:
                                w[i], w[i + step] = swap(v[i], v[i + step], shift, mask)
                        v = w
                        step //= 2
                    row = c * lines + r * line_dev
                    x_ref[row : row + line_dev, j * LANES : (j + 1) * LANES] = (
                        jnp.concatenate(v, axis=0).astype(bf16)
                    )
        for s in range(0, narrow, width):
            pixels = x_ref[s * lines : (s + width) * lines, :]
            both = jnp.dot(pixels, keep_ref[:bands], preferred_element_type=f32)
            both = both + jnp.dot(pixels, keep_ref[bands:], preferred_element_type=f32)
            res_ref[s : s + width] = both.astype(bf16).reshape(width, lines, bands)
            found = contract_last(gain_ref[...], pixels)
            found = found[:kept] + found[kept:]
            for i in range(width):
                hold_ref[:, s + i, :] = found[:, i * lines : (i + 1) * lines]
        coef_ref[...] = hold_ref[...].astype(bf16)

    return pl.pallas_call(
        kernel,
        out_shape=(
            jax.ShapeDtypeStruct((narrow, lines, bands), bf16),
            jax.ShapeDtypeStruct((kept, narrow, lines), bf16),
        ),
        scratch_shapes=[
            pltpu.VMEM((sources * (rows // LANES), narrow, LANES), f32),
            pltpu.VMEM((narrow * lines, bands), bf16),
            pltpu.VMEM((kept, narrow, lines), f32),
        ],
        name="finish",
    )(pltpu.with_memory_space_constraint(arrived, pltpu.VMEM), keep, gains)


def exchange(x, axis, k):
    count = lax.axis_size(axis)
    return lax.ppermute(x, axis, [(i, i ^ k) for i in range(count)])


def split(a):
    high = lax.reduce_precision(a, 8, 7)
    return jnp.concatenate([high, a - high], axis=0).astype(bf16)


def orthonormal(spectra):
    gram = jnp.dot(spectra, spectra.T, precision=highest)
    factor = jnp.linalg.cholesky(gram)
    return jax.scipy.linalg.solve_triangular(factor, spectra, lower=True)


def operators(basis):
    count = basis.shape[0] // 2
    first = basis[:count]
    second = basis[count:]
    cross = jnp.dot(second, first.T, precision=highest)
    second_gain = second - jnp.dot(cross, first, precision=highest)
    gains = jnp.concatenate([first, second_gain], axis=0)
    keep = jnp.eye(basis.shape[1], dtype=f32) - jnp.dot(gains.T, basis, precision=highest)
    return keep, gains


def project(block, basis):
    count = basis.shape[0] // 2
    first = basis[:count]
    second = basis[count:]
    coef_one = jnp.einsum("clb,kb->kcl", block, first, precision=highest)
    remain = block - jnp.einsum("kcl,kb->clb", coef_one, first, precision=highest)
    coef_two = jnp.einsum("clb,kb->kcl", remain, second, precision=highest)
    remain = remain - jnp.einsum("kcl,kb->clb", coef_two, second, precision=highest)
    return (
        remain.astype(bf16),
        jnp.concatenate([coef_one, coef_two], axis=0).astype(bf16),
    )


def plain(band_images, line_index, column, pix_count, row_count, narrow):
    band_dev, line_dev, cols_all = band_images.shape
    offset = line_index - lax.axis_index("row") * line_dev
    inside = (offset >= 0) & (offset < line_dev)
    position = jnp.clip(offset, 0, line_dev - 1) * cols_all + column
    picked = jnp.take(band_images.reshape(band_dev, line_dev * cols_all), position, axis=1)
    picked = jnp.where(inside[None, :], picked, jnp.zeros_like(picked))
    stacked = lax.all_gather(picked, "pix", axis=0, tiled=True)
    spectra = lax.psum(stacked.astype(f32).astype(bf16), "row").astype(f32)
    basis = orthonormal(spectra.T)
    shaped = band_images.reshape(band_dev, line_dev, pix_count, row_count, narrow)
    arrived = lax.all_to_all(
        lax.all_to_all(shaped, "pix", split_axis=2, concat_axis=0, tiled=True),
        "row",
        split_axis=3,
        concat_axis=1,
        tiled=True,
    )
    block = (
        arrived.reshape(arrived.shape[0], arrived.shape[1], narrow)
        .transpose(2, 1, 0)
        .astype(f32)
    )
    return project(block, basis)


def shards(band_images, pivots):
    band_dev, line_dev, cols_all = band_images.shape
    pix_count = lax.axis_size("pix")
    row_count = lax.axis_size("row")
    part_count = pix_count * row_count
    narrow = cols_all // part_count
    flat_pivots = pivots.reshape(-1)
    pivot_count = flat_pivots.shape[0]
    line_index = flat_pivots // cols_all
    column = flat_pivots % cols_all
    lines = row_count * line_dev
    bands = pix_count * band_dev
    taken = LANES // band_dev
    fits = (
        taken * band_dev == LANES
        and taken in (1, 2, 4, 8)
        and line_dev == SUBLANES * taken
        and narrow % 16 == 0
        and cols_all % (2 * LANES) == 0
        and lines == LANES
        and bands % LANES == 0
        and cols_all & (cols_all - 1) == 0
        and pix_count & (pix_count - 1) == 0
        and row_count & (row_count - 1) == 0
    )
    if not fits:
        return plain(band_images, line_index, column, pix_count, row_count, narrow)
    row_index = lax.axis_index("row").astype(jnp.int32).reshape(1)
    picked = pick(band_images, pivots, row_index)
    found = picked
    for k in range(1, row_count):
        found = found + exchange(picked, "row", k)
    packed = pack(band_images).reshape(part_count, narrow, line_dev * band_dev)
    arrived = lax.all_to_all(packed, AXES, 0, 0, tiled=True)
    order = found[None]
    for k in range(pix_count.bit_length() - 1):
        order = jnp.concatenate([order, exchange(order, "pix", 1 << k)], axis=0)
    spectra = order.astype(f32)[jnp.arange(pix_count) ^ lax.axis_index("pix")]
    spectra = spectra.reshape(bands, pivot_count).T
    keep, gains = operators(orthonormal(spectra))
    keep, gains = split(keep), split(gains)
    return finish(arrived, keep, gains, pix_count, row_count, band_dev, line_dev)


def solution(mesh):
    placed = (P("pix", "row", None), P())
    return jax.shard_map(
        shards,
        mesh=mesh,
        in_specs=placed,
        out_specs=(P(AXES, None, None), P(None, AXES, None)),
        check_vma=False,
    )
```

```python
import jax
import jax.numpy as jnp
from jax import lax
from jax.experimental import pallas as pl
from jax.experimental.pallas import tpu as pltpu
from jax.sharding import PartitionSpec as P


highest = lax.Precision.HIGHEST
f32 = jnp.float32
bf16 = jnp.bfloat16
LANES = 128
SUBLANES = 8
AXES = ("pix", "row")


def contract_last(a, b):
    return lax.dot_general(a, b, (((1,), (1,)), ((), ())), preferred_element_type=f32)


def hot(shape, test):
    row = lax.broadcasted_iota(jnp.int32, shape, 0)
    column = lax.broadcasted_iota(jnp.int32, shape, 1)
    return test(row, column).astype(f32).astype(bf16)


def swap_rows(outer, inner):
    size = outer * inner
    return hot((size, size), lambda m, r: r == (m % outer) * inner + m // outer)


def pick(band_images, pivots, row_index):
    band_dev, line_dev, cols = band_images.shape
    panels, panel = pivots.shape
    pivot_count = panels * panel
    shift = cols.bit_length() - 1
    chunks = 4
    step = band_dev // chunks
    rows = step * line_dev

    def kernel(row_ref, x_ref, piv_ref, spec_ref, held_ref, sems):
        def copy(i):
            part = slice(i * step, (i + 1) * step)
            return pltpu.make_async_copy(x_ref.at[part], held_ref.at[part], sems.at[i])

        for i in range(chunks):
            copy(i).start()
        flat = jnp.concatenate([piv_ref[i : i + 1, :] for i in range(panels)], axis=1).astype(f32)
        own = lax.broadcasted_iota(jnp.int32, (pivot_count, pivot_count), 0) == lax.broadcasted_iota(
            jnp.int32, (pivot_count, pivot_count), 1
        )
        flat = jnp.sum(jnp.where(own, flat, 0.0), axis=1, keepdims=True).astype(jnp.int32)
        column = flat & (cols - 1)
        inner = (flat >> shift) - row_ref[0] * line_dev
        chosen = hot((pivot_count, cols), lambda k, c: c == column)
        lane = lax.broadcasted_iota(jnp.int32, (pivot_count, rows), 1)
        inside = lane % line_dev == inner
        fold = hot((step, rows), lambda b, r: r // line_dev == b)
        for i in range(chunks):
            copy(i).wait()
            part = held_ref[i * step : (i + 1) * step].reshape(rows, cols)
            found = jnp.where(inside, contract_last(chosen, part), 0.0).astype(bf16)
            spec_ref[i * step : (i + 1) * step, :] = contract_last(fold, found).astype(bf16)

    return pl.pallas_call(
        kernel,
        out_shape=jax.ShapeDtypeStruct((band_dev, pivot_count), bf16),
        in_specs=[
            pl.BlockSpec(memory_space=pltpu.SMEM),
            pl.BlockSpec(memory_space=pl.ANY),
            pl.BlockSpec(memory_space=pltpu.VMEM),
        ],
        scratch_shapes=[pltpu.VMEM(band_images.shape, bf16), pltpu.SemaphoreType.DMA((chunks,))],
        name="pick",
    )(row_index, band_images, pivots)


def pack(band_images):
    band_dev, line_dev, cols = band_images.shape
    rows = band_dev * line_dev
    taken = LANES // band_dev
    groups = line_dev // taken
    wide = SUBLANES * line_dev
    sides = cols // wide

    def kernel(x_ref, out_ref, held_ref, rows_ref, out_buf, in_sems, out_sems):
        def take(j):
            part = pl.ds(j * wide, wide)
            return pltpu.make_async_copy(x_ref.at[:, :, part], held_ref.at[:, :, part], in_sems.at[j])

        def give(j):
            part = pl.ds(j * wide, wide)
            return pltpu.make_async_copy(out_buf.at[part], out_ref.at[part], out_sems.at[j])

        for j in range(sides):
            take(j).start()
        eye = hot((wide, wide), lambda m, r: m == r)
        mixed = swap_rows(SUBLANES, line_dev)
        for j in range(sides):
            take(j).wait()
            side = slice(j * wide, (j + 1) * wide)
            for i in range(0, band_dev, 2 * SUBLANES):
                low, high = (
                    jnp.dot(
                        mixed,
                        held_ref[k : k + SUBLANES, :, side].reshape(wide, wide),
                        preferred_element_type=f32,
                    )
                    for k in (i, i + SUBLANES)
                )
                for line in range(line_dev):
                    start = ((line % groups) * taken + line // groups) * band_dev + i
                    at = slice(line * SUBLANES, (line + 1) * SUBLANES)
                    rows_ref[start : start + 2 * SUBLANES, side] = jnp.concatenate(
                        [low[at], high[at]], axis=0
                    ).astype(bf16)
            out_buf[side, :] = contract_last(eye, rows_ref[:, side]).astype(bf16)
            give(j).start()
        for j in range(sides):
            give(j).wait()

    return pl.pallas_call(
        kernel,
        out_shape=jax.ShapeDtypeStruct((cols, rows), bf16),
        in_specs=[pl.BlockSpec(memory_space=pl.ANY)],
        out_specs=pl.BlockSpec(memory_space=pl.ANY),
        scratch_shapes=[
            pltpu.VMEM(band_images.shape, bf16),
            pltpu.VMEM((rows, cols), bf16),
            pltpu.VMEM((cols, rows), bf16),
            pltpu.SemaphoreType.DMA((sides,)),
            pltpu.SemaphoreType.DMA((sides,)),
        ],
        name="pack",
    )(band_images)


def finish(arrived, keep, gains, pix_count, row_count, band_dev, line_dev):
    _, narrow, _ = arrived.shape
    taken = LANES // band_dev
    groups = line_dev // taken
    lines = row_count * line_dev
    bands = pix_count * band_dev
    kept = gains.shape[0] // 2
    width = 4
    joined = bands // LANES
    pieces = narrow // width

    def swap(low, high, shift, mask):
        return (
            jnp.where(mask, low, pltpu.roll(high, shift, 1)),
            jnp.where(mask, pltpu.roll(low, LANES - shift, 1), high),
        )

    def kernel(a_ref, keep_ref, gain_ref, res_ref, coef_ref, x_ref, hold_ref, res_buf, coef_buf, sems):
        def give(i):
            part = pl.ds(i * width, width)
            return pltpu.make_async_copy(res_buf.at[part], res_ref.at[part], sems.at[i])

        last = pltpu.make_async_copy(coef_buf, coef_ref, sems.at[pieces])
        lane = lax.broadcasted_iota(jnp.int32, (SUBLANES, LANES), 1)
        half = groups * narrow
        mixed = hot(
            (2 * half, 2 * half),
            lambda m, r: r == (m // half) * half + (m % groups) * narrow + (m % half) // groups,
        )
        for r in range(row_count):
            for j in range(joined):
                sides = []
                for n in range(taken // 2):
                    tall = []
                    for s in range(2):
                        source = (j * taken + s * (taken // 2) + n) * row_count + r
                        tall += [a_ref[source, :, g * LANES : (g + 1) * LANES] for g in range(groups)]
                    sides.append(jnp.concatenate(tall, axis=0))
                turned = jnp.dot(mixed, jnp.concatenate(sides, axis=1), preferred_element_type=f32)
                for c in range(narrow):
                    v = []
                    for i in range(taken):
                        s, n = i // (taken // 2), i % (taken // 2)
                        start = (s * narrow + c) * groups
                        v.append(turned[start : start + groups, n * LANES : (n + 1) * LANES])
                    step = taken // 2
                    while step >= 1:
                        shift = step * band_dev
                        mask = (lane // shift) % 2 == 0
                        w = list(v)
                        for i in range(taken):
                            if (i // step) % 2 == 0:
                                w[i], w[i + step] = swap(v[i], v[i + step], shift, mask)
                        v = w
                        step //= 2
                    row = c * lines + r * line_dev
                    x_ref[row : row + line_dev, j * LANES : (j + 1) * LANES] = (
                        jnp.concatenate(v, axis=0).astype(bf16)
                    )
        for c in range(0, narrow, 2):
            found = contract_last(gain_ref[...], x_ref[c * lines : (c + 2) * lines, :])
            found = (found[:kept] + found[kept:]).astype(bf16)
            hold_ref[c] = found[:, :lines]
            hold_ref[c + 1] = found[:, lines:]
        turn = swap_rows(narrow, narrow)
        for k in range(0, kept, 2 * narrow):
            tall = [
                jnp.concatenate([hold_ref[c, q : q + narrow, :] for c in range(narrow)], axis=0)
                for q in (k, k + narrow)
            ]
            turned = jnp.dot(turn, jnp.concatenate(tall, axis=1), preferred_element_type=f32).astype(bf16)
            coef_buf[k : k + narrow] = turned[:, :lines].reshape(narrow, narrow, lines)
            coef_buf[k + narrow : k + 2 * narrow] = turned[:, lines:].reshape(narrow, narrow, lines)
        last.start()
        for p in range(pieces):
            pixels = x_ref[p * width * lines : (p + 1) * width * lines, :]
            both = jnp.dot(pixels, keep_ref[:bands], preferred_element_type=f32)
            both = both + jnp.dot(pixels, keep_ref[bands:], preferred_element_type=f32)
            res_buf[p * width : (p + 1) * width] = both.astype(bf16).reshape(width, lines, bands)
            give(p).start()
        last.wait()
        for p in range(pieces):
            give(p).wait()

    near = [pltpu.with_memory_space_constraint(v, pltpu.VMEM) for v in (arrived, keep, gains)]
    return pl.pallas_call(
        kernel,
        out_shape=(
            jax.ShapeDtypeStruct((narrow, lines, bands), bf16),
            jax.ShapeDtypeStruct((kept, narrow, lines), bf16),
        ),
        out_specs=(pl.BlockSpec(memory_space=pl.ANY), pl.BlockSpec(memory_space=pl.ANY)),
        scratch_shapes=[
            pltpu.VMEM((narrow * lines, bands), bf16),
            pltpu.VMEM((narrow, kept, lines), bf16),
            pltpu.VMEM((narrow, lines, bands), bf16),
            pltpu.VMEM((kept, narrow, lines), bf16),
            pltpu.SemaphoreType.DMA((pieces + 1,)),
        ],
        name="finish",
    )(*near)


def factor(spectra):
    bands, count = spectra.shape
    half = count // 2

    def kernel(s_ref, keep_ref, gain_ref):
        s = s_ref[...].astype(f32)
        st = s.T
        gram = jnp.dot(st, s, precision=highest, preferred_element_type=f32)
        row = lax.broadcasted_iota(jnp.int32, (count, 2 * count), 0)
        lane = lax.broadcasted_iota(jnp.int32, (count, 2 * count), 1)
        both = jnp.concatenate([gram, jnp.where(lane == row, 1.0, 0.0)[:, :count]], axis=1)
        done = []
        for j in range(count):
            base = j // SUBLANES * SUBLANES
            scale = 1.0 / jnp.sqrt(both[j - base : j - base + 1, j : j + 1])
            top = both[j - base : j - base + 1, :] * scale
            done.append(top[:, count:])
            if (j + 1) % SUBLANES == 0:
                both = both[SUBLANES:]
            if j + 1 < count:
                column = both[:, j : j + 1] * scale
                both = both - column * top
        inverse = jnp.concatenate(done, axis=0)
        basis = jnp.dot(inverse, st, precision=highest, preferred_element_type=f32)
        tall = basis.T
        cross = lax.dot_general(
            basis[:half], basis[half:], (((1,), (1,)), ((), ())), precision=highest, preferred_element_type=f32
        )
        second = tall[:, half:] - jnp.dot(tall[:, :half], cross, precision=highest, preferred_element_type=f32)
        gains = jnp.concatenate([tall[:, :half], second], axis=1)
        keep = jnp.where(
            lax.broadcasted_iota(jnp.int32, (bands, bands), 0)
            == lax.broadcasted_iota(jnp.int32, (bands, bands), 1),
            1.0,
            0.0,
        ) - jnp.dot(gains, basis, precision=highest, preferred_element_type=f32)
        gains = gains.T
        for ref, value, size in ((keep_ref, keep, bands), (gain_ref, gains, count)):
            high = value.astype(bf16)
            ref[:size] = high
            ref[size:] = (value - high.astype(f32)).astype(bf16)

    return pl.pallas_call(
        kernel,
        out_shape=(
            pltpu.VMEM((2 * bands, bands), bf16),
            pltpu.VMEM((2 * count, bands), bf16),
        ),
        name="factor",
    )(spectra)


def exchange(x, axis, k):
    count = lax.axis_size(axis)
    return lax.ppermute(x, axis, [(i, i ^ k) for i in range(count)])


def orthonormal(spectra):
    gram = jnp.dot(spectra, spectra.T, precision=highest)
    factor = jnp.linalg.cholesky(gram)
    return jax.scipy.linalg.solve_triangular(factor, spectra, lower=True)


def project(block, basis):
    count = basis.shape[0] // 2
    first = basis[:count]
    second = basis[count:]
    coef_one = jnp.einsum("clb,kb->kcl", block, first, precision=highest)
    remain = block - jnp.einsum("kcl,kb->clb", coef_one, first, precision=highest)
    coef_two = jnp.einsum("clb,kb->kcl", remain, second, precision=highest)
    remain = remain - jnp.einsum("kcl,kb->clb", coef_two, second, precision=highest)
    return (
        remain.astype(bf16),
        jnp.concatenate([coef_one, coef_two], axis=0).astype(bf16),
    )


def plain(band_images, line_index, column, pix_count, row_count, narrow):
    band_dev, line_dev, cols_all = band_images.shape
    offset = line_index - lax.axis_index("row") * line_dev
    inside = (offset >= 0) & (offset < line_dev)
    position = jnp.clip(offset, 0, line_dev - 1) * cols_all + column
    picked = jnp.take(band_images.reshape(band_dev, line_dev * cols_all), position, axis=1)
    picked = jnp.where(inside[None, :], picked, jnp.zeros_like(picked))
    stacked = lax.all_gather(picked, "pix", axis=0, tiled=True)
    spectra = lax.psum(stacked.astype(f32).astype(bf16), "row").astype(f32)
    basis = orthonormal(spectra.T)
    shaped = band_images.reshape(band_dev, line_dev, pix_count, row_count, narrow)
    arrived = lax.all_to_all(
        lax.all_to_all(shaped, "pix", split_axis=2, concat_axis=0, tiled=True),
        "row",
        split_axis=3,
        concat_axis=1,
        tiled=True,
    )
    block = (
        arrived.reshape(arrived.shape[0], arrived.shape[1], narrow)
        .transpose(2, 1, 0)
        .astype(f32)
    )
    return project(block, basis)


def shards(band_images, pivots):
    band_dev, line_dev, cols_all = band_images.shape
    pix_count = lax.axis_size("pix")
    row_count = lax.axis_size("row")
    part_count = pix_count * row_count
    narrow = cols_all // part_count
    flat_pivots = pivots.reshape(-1)
    pivot_count = flat_pivots.shape[0]
    line_index = flat_pivots // cols_all
    column = flat_pivots % cols_all
    lines = row_count * line_dev
    bands = pix_count * band_dev
    taken = LANES // band_dev
    fits = (
        taken * band_dev == LANES
        and taken in (2, 4)
        and line_dev == SUBLANES * taken
        and narrow == 16
        and cols_all % (SUBLANES * line_dev) == 0
        and lines == LANES
        and 2 * pivot_count == LANES
        and bands % LANES == 0
        and cols_all & (cols_all - 1) == 0
        and pix_count & (pix_count - 1) == 0
        and row_count & (row_count - 1) == 0
    )
    if not fits:
        return plain(band_images, line_index, column, pix_count, row_count, narrow)
    row_index = lax.axis_index("row").astype(jnp.int32).reshape(1)
    picked = pick(band_images, pivots, row_index)
    found = picked
    for k in range(1, row_count):
        found = found + exchange(picked, "row", k)
    packed = pack(band_images).reshape(part_count, narrow, line_dev * band_dev)
    arrived = lax.all_to_all(packed, AXES, 0, 0, tiled=True)
    for k in range(pix_count.bit_length() - 1):
        other = exchange(found, "pix", 1 << k)
        after = (lax.axis_index("pix") >> k) % 2 == 1
        found = jnp.where(after, jnp.concatenate([other, found], axis=0), jnp.concatenate([found, other], axis=0))
    keep, gains = factor(found)
    return finish(arrived, keep, gains, pix_count, row_count, band_dev, line_dev)


def solution(mesh):
    placed = (P("pix", "row", None), P())
    return jax.shard_map(
        shards,
        mesh=mesh,
        in_specs=placed,
        out_specs=(P(AXES, None, None), P(None, AXES, None)),
        check_vma=False,
    )
```

```python
import jax
import jax.numpy as jnp
from jax import lax
from jax.experimental import pallas as pl
from jax.experimental.pallas import tpu as pltpu
from jax.sharding import PartitionSpec as P


highest = lax.Precision.HIGHEST
f32 = jnp.float32
bf16 = jnp.bfloat16
LANES = 128
SUBLANES = 8
AXES = ("pix", "row")


def contract_last(a, b):
    return lax.dot_general(a, b, (((1,), (1,)), ((), ())), preferred_element_type=f32)


def hot(shape, test):
    row = lax.broadcasted_iota(jnp.int32, shape, 0)
    column = lax.broadcasted_iota(jnp.int32, shape, 1)
    return test(row, column).astype(f32).astype(bf16)


def swap_rows(outer, inner):
    size = outer * inner
    return hot((size, size), lambda m, r: r == (m % outer) * inner + m // outer)


def pick(band_images, pivots):
    band_dev, line_dev, cols = band_images.shape
    panels, panel = pivots.shape
    pivot_count = panels * panel
    shift = cols.bit_length() - 1
    chunks = 4
    step = band_dev // chunks
    rows = step * line_dev

    def kernel(x_ref, far_ref, held_ref, spec_ref, piv_ref, sems):
        def copy(i):
            part = pl.ds(i * step, step)
            return pltpu.make_async_copy(x_ref.at[part], held_ref.at[part], sems.at[i])

        indices = pltpu.make_async_copy(far_ref, piv_ref, sems.at[chunks])
        indices.start()
        for i in range(chunks):
            copy(i).start()
        indices.wait()
        flat = jnp.concatenate([piv_ref[i : i + 1, :] for i in range(panels)], axis=1).astype(f32)
        own = lax.broadcasted_iota(jnp.int32, (pivot_count, pivot_count), 0) == lax.broadcasted_iota(
            jnp.int32, (pivot_count, pivot_count), 1
        )
        flat = jnp.sum(jnp.where(own, flat, 0.0), axis=1, keepdims=True).astype(jnp.int32)
        column = flat & (cols - 1)
        inner = (flat >> shift) - lax.axis_index("row").astype(jnp.int32) * line_dev
        chosen = hot((pivot_count, cols), lambda k, c: c == column)
        lane = lax.broadcasted_iota(jnp.int32, (pivot_count, rows), 1)
        inside = lane % line_dev == inner
        fold = hot((step, rows), lambda b, r: r // line_dev == b)
        for i in range(chunks):
            copy(i).wait()
            part = held_ref[i * step : (i + 1) * step].reshape(rows, cols)
            found = jnp.where(inside, contract_last(chosen, part), 0.0).astype(bf16)
            spec_ref[i * step : (i + 1) * step, :] = contract_last(fold, found).astype(bf16)

    return pl.pallas_call(
        kernel,
        out_shape=(
            pltpu.VMEM(band_images.shape, bf16),
            pltpu.VMEM((band_dev, pivot_count), bf16),
        ),
        in_specs=[pl.BlockSpec(memory_space=pl.ANY), pl.BlockSpec(memory_space=pl.ANY)],
        scratch_shapes=[pltpu.VMEM(pivots.shape, pivots.dtype), pltpu.SemaphoreType.DMA((chunks + 1,))],
        name="pick",
    )(band_images, pivots)


def pack(band_images):
    band_dev, line_dev, cols = band_images.shape
    rows = band_dev * line_dev
    taken = LANES // band_dev
    groups = line_dev // taken
    wide = SUBLANES * line_dev
    sides = cols // wide

    def kernel(x_ref, out_ref, rows_ref, out_buf, sems):
        def give(j, q):
            part = (pl.ds(j * wide, wide), pl.ds(q * wide, wide))
            return pltpu.make_async_copy(out_buf.at[part], out_ref.at[part], sems.at[j, q])

        eye = hot((wide, wide), lambda m, r: m == r)
        mixed = swap_rows(SUBLANES, line_dev)
        for j in range(sides):
            side = slice(j * wide, (j + 1) * wide)
            for i in range(0, band_dev, 2 * SUBLANES):
                low, high = (
                    jnp.dot(
                        mixed,
                        x_ref[k : k + SUBLANES, :, side].reshape(wide, wide),
                        preferred_element_type=f32,
                    )
                    for k in (i, i + SUBLANES)
                )
                for line in range(line_dev):
                    start = ((line % groups) * taken + line // groups) * band_dev + i
                    at = slice(line * SUBLANES, (line + 1) * SUBLANES)
                    rows_ref[start : start + 2 * SUBLANES, side] = jnp.concatenate(
                        [low[at], high[at]], axis=0
                    ).astype(bf16)
            for q in range(rows // wide):
                part = slice(q * wide, (q + 1) * wide)
                out_buf[side, part] = contract_last(eye, rows_ref[part, side]).astype(bf16)
                give(j, q).start()
        for j in range(sides):
            for q in range(rows // wide):
                give(j, q).wait()

    return pl.pallas_call(
        kernel,
        out_shape=jax.ShapeDtypeStruct((cols, rows), bf16),
        in_specs=[pl.BlockSpec(memory_space=pltpu.VMEM)],
        out_specs=pl.BlockSpec(memory_space=pl.ANY),
        scratch_shapes=[
            pltpu.VMEM((rows, cols), bf16),
            pltpu.VMEM((cols, rows), bf16),
            pltpu.SemaphoreType.DMA((sides, rows // wide)),
        ],
        name="pack",
    )(pltpu.with_memory_space_constraint(band_images, pltpu.VMEM))


def finish(arrived, keep, gains, pix_count, row_count, band_dev, line_dev):
    _, narrow, _ = arrived.shape
    taken = LANES // band_dev
    groups = line_dev // taken
    lines = row_count * line_dev
    bands = pix_count * band_dev
    kept = gains.shape[0] // 2
    width = 4
    joined = bands // LANES
    pieces = narrow // width

    def swap(low, high, shift, mask):
        return (
            jnp.where(mask, low, pltpu.roll(high, shift, 1)),
            jnp.where(mask, pltpu.roll(low, LANES - shift, 1), high),
        )

    def kernel(a_ref, keep_ref, gain_ref, res_ref, coef_ref, x_ref, hold_ref, res_buf, coef_buf, sems):
        def give(i):
            part = pl.ds(i * width, width)
            return pltpu.make_async_copy(res_buf.at[part], res_ref.at[part], sems.at[i])

        last = pltpu.make_async_copy(coef_buf, coef_ref, sems.at[pieces])
        lane = lax.broadcasted_iota(jnp.int32, (SUBLANES, LANES), 1)
        half = groups * narrow
        mixed = hot(
            (2 * half, 2 * half),
            lambda m, r: r == (m // half) * half + (m % groups) * narrow + (m % half) // groups,
        )
        for r in range(row_count):
            for j in range(joined):
                sides = []
                for n in range(taken // 2):
                    tall = []
                    for s in range(2):
                        source = (j * taken + s * (taken // 2) + n) * row_count + r
                        tall += [a_ref[source, :, g * LANES : (g + 1) * LANES] for g in range(groups)]
                    sides.append(jnp.concatenate(tall, axis=0))
                turned = jnp.dot(mixed, jnp.concatenate(sides, axis=1), preferred_element_type=f32)
                for c in range(narrow):
                    v = []
                    for i in range(taken):
                        s, n = i // (taken // 2), i % (taken // 2)
                        start = (s * narrow + c) * groups
                        v.append(turned[start : start + groups, n * LANES : (n + 1) * LANES])
                    step = taken // 2
                    while step >= 1:
                        shift = step * band_dev
                        mask = (lane // shift) % 2 == 0
                        w = list(v)
                        for i in range(taken):
                            if (i // step) % 2 == 0:
                                w[i], w[i + step] = swap(v[i], v[i + step], shift, mask)
                        v = w
                        step //= 2
                    row = c * lines + r * line_dev
                    x_ref[row : row + line_dev, j * LANES : (j + 1) * LANES] = (
                        jnp.concatenate(v, axis=0).astype(bf16)
                    )
        for c in range(0, narrow, 2):
            found = contract_last(gain_ref[...], x_ref[c * lines : (c + 2) * lines, :])
            found = (found[:kept] + found[kept:]).astype(bf16)
            hold_ref[c] = found[:, :lines]
            hold_ref[c + 1] = found[:, lines:]
        turn = swap_rows(narrow, narrow)
        for k in range(0, kept, 2 * narrow):
            tall = [
                jnp.concatenate([hold_ref[c, q : q + narrow, :] for c in range(narrow)], axis=0)
                for q in (k, k + narrow)
            ]
            turned = jnp.dot(turn, jnp.concatenate(tall, axis=1), preferred_element_type=f32).astype(bf16)
            coef_buf[k : k + narrow] = turned[:, :lines].reshape(narrow, narrow, lines)
            coef_buf[k + narrow : k + 2 * narrow] = turned[:, lines:].reshape(narrow, narrow, lines)
        last.start()
        for p in range(pieces):
            pixels = x_ref[p * width * lines : (p + 1) * width * lines, :]
            both = jnp.dot(pixels, keep_ref[:bands], preferred_element_type=f32)
            both = both + jnp.dot(pixels, keep_ref[bands:], preferred_element_type=f32)
            res_buf[p * width : (p + 1) * width] = both.astype(bf16).reshape(width, lines, bands)
            give(p).start()
        last.wait()
        for p in range(pieces):
            give(p).wait()

    near = [pltpu.with_memory_space_constraint(v, pltpu.VMEM) for v in (arrived, keep, gains)]
    return pl.pallas_call(
        kernel,
        out_shape=(
            jax.ShapeDtypeStruct((narrow, lines, bands), bf16),
            jax.ShapeDtypeStruct((kept, narrow, lines), bf16),
        ),
        out_specs=(pl.BlockSpec(memory_space=pl.ANY), pl.BlockSpec(memory_space=pl.ANY)),
        scratch_shapes=[
            pltpu.VMEM((narrow * lines, bands), bf16),
            pltpu.VMEM((narrow, kept, lines), bf16),
            pltpu.VMEM((narrow, lines, bands), bf16),
            pltpu.VMEM((kept, narrow, lines), bf16),
            pltpu.SemaphoreType.DMA((pieces + 1,)),
        ],
        name="finish",
    )(*near)


def factor(spectra):
    bands, count = spectra.shape
    half = count // 2

    def kernel(s_ref, keep_ref, gain_ref):
        s = s_ref[...].astype(f32)
        st = s.T
        gram = jnp.dot(st, s, precision=highest, preferred_element_type=f32)
        row = lax.broadcasted_iota(jnp.int32, (count, 2 * count), 0)
        lane = lax.broadcasted_iota(jnp.int32, (count, 2 * count), 1)
        both = jnp.concatenate([gram, jnp.where(lane == row, 1.0, 0.0)[:, :count]], axis=1)
        done = []
        for j in range(count):
            base = j // SUBLANES * SUBLANES
            scale = 1.0 / jnp.sqrt(both[j - base : j - base + 1, j : j + 1])
            top = both[j - base : j - base + 1, :] * scale
            done.append(top[:, count:])
            if (j + 1) % SUBLANES == 0:
                both = both[SUBLANES:]
            if j + 1 < count:
                column = both[:, j : j + 1] * scale
                both = both - column * top
        inverse = jnp.concatenate(done, axis=0)
        basis = jnp.dot(inverse, st, precision=highest, preferred_element_type=f32)
        tall = basis.T
        cross = lax.dot_general(
            basis[:half], basis[half:], (((1,), (1,)), ((), ())), precision=highest, preferred_element_type=f32
        )
        second = tall[:, half:] - jnp.dot(tall[:, :half], cross, precision=highest, preferred_element_type=f32)
        gains = jnp.concatenate([tall[:, :half], second], axis=1)
        keep = jnp.where(
            lax.broadcasted_iota(jnp.int32, (bands, bands), 0)
            == lax.broadcasted_iota(jnp.int32, (bands, bands), 1),
            1.0,
            0.0,
        ) - jnp.dot(gains, basis, precision=highest, preferred_element_type=f32)
        gains = gains.T
        for ref, value, size in ((keep_ref, keep, bands), (gain_ref, gains, count)):
            high = value.astype(bf16)
            ref[:size] = high
            ref[size:] = (value - high.astype(f32)).astype(bf16)

    return pl.pallas_call(
        kernel,
        out_shape=(
            pltpu.VMEM((2 * bands, bands), bf16),
            pltpu.VMEM((2 * count, bands), bf16),
        ),
        name="factor",
    )(spectra)


def exchange(x, axis, k):
    count = lax.axis_size(axis)
    return lax.ppermute(x, axis, [(i, i ^ k) for i in range(count)])


def orthonormal(spectra):
    gram = jnp.dot(spectra, spectra.T, precision=highest)
    factor = jnp.linalg.cholesky(gram)
    return jax.scipy.linalg.solve_triangular(factor, spectra, lower=True)


def project(block, basis):
    count = basis.shape[0] // 2
    first = basis[:count]
    second = basis[count:]
    coef_one = jnp.einsum("clb,kb->kcl", block, first, precision=highest)
    remain = block - jnp.einsum("kcl,kb->clb", coef_one, first, precision=highest)
    coef_two = jnp.einsum("clb,kb->kcl", remain, second, precision=highest)
    remain = remain - jnp.einsum("kcl,kb->clb", coef_two, second, precision=highest)
    return (
        remain.astype(bf16),
        jnp.concatenate([coef_one, coef_two], axis=0).astype(bf16),
    )


def plain(band_images, line_index, column, pix_count, row_count, narrow):
    band_dev, line_dev, cols_all = band_images.shape
    offset = line_index - lax.axis_index("row") * line_dev
    inside = (offset >= 0) & (offset < line_dev)
    position = jnp.clip(offset, 0, line_dev - 1) * cols_all + column
    picked = jnp.take(band_images.reshape(band_dev, line_dev * cols_all), position, axis=1)
    picked = jnp.where(inside[None, :], picked, jnp.zeros_like(picked))
    stacked = lax.all_gather(picked, "pix", axis=0, tiled=True)
    spectra = lax.psum(stacked.astype(f32).astype(bf16), "row").astype(f32)
    basis = orthonormal(spectra.T)
    shaped = band_images.reshape(band_dev, line_dev, pix_count, row_count, narrow)
    arrived = lax.all_to_all(
        lax.all_to_all(shaped, "pix", split_axis=2, concat_axis=0, tiled=True),
        "row",
        split_axis=3,
        concat_axis=1,
        tiled=True,
    )
    block = (
        arrived.reshape(arrived.shape[0], arrived.shape[1], narrow)
        .transpose(2, 1, 0)
        .astype(f32)
    )
    return project(block, basis)


def shards(band_images, pivots):
    band_dev, line_dev, cols_all = band_images.shape
    pix_count = lax.axis_size("pix")
    row_count = lax.axis_size("row")
    part_count = pix_count * row_count
    narrow = cols_all // part_count
    flat_pivots = pivots.reshape(-1)
    pivot_count = flat_pivots.shape[0]
    line_index = flat_pivots // cols_all
    column = flat_pivots % cols_all
    lines = row_count * line_dev
    bands = pix_count * band_dev
    taken = LANES // band_dev
    fits = (
        taken * band_dev == LANES
        and taken in (2, 4)
        and line_dev == SUBLANES * taken
        and narrow == 16
        and cols_all % (SUBLANES * line_dev) == 0
        and lines == LANES
        and 2 * pivot_count == LANES
        and bands % LANES == 0
        and cols_all & (cols_all - 1) == 0
        and pix_count & (pix_count - 1) == 0
        and row_count & (row_count - 1) == 0
    )
    if not fits:
        return plain(band_images, line_index, column, pix_count, row_count, narrow)
    held, picked = pick(band_images, pivots)
    found = picked
    for k in range(row_count.bit_length() - 1):
        found = found + exchange(found, "row", 1 << k)
    packed = pack(held).reshape(part_count, narrow, line_dev * band_dev)
    arrived = lax.all_to_all(packed, AXES, 0, 0, tiled=True)
    for k in range(pix_count.bit_length() - 1):
        other = exchange(found, "pix", 1 << k)
        after = (lax.axis_index("pix") >> k) % 2 == 1
        found = jnp.where(after, jnp.concatenate([other, found], axis=0), jnp.concatenate([found, other], axis=0))
    keep, gains = factor(found)
    return finish(arrived, keep, gains, pix_count, row_count, band_dev, line_dev)


def solution(mesh):
    placed = (P("pix", "row", None), P())
    return jax.shard_map(
        shards,
        mesh=mesh,
        in_specs=placed,
        out_specs=(P(AXES, None, None), P(None, AXES, None)),
        check_vma=False,
    )
```

```python
import jax
import jax.numpy as jnp
from jax import lax
from jax.experimental import pallas as pl
from jax.experimental.pallas import tpu as pltpu
from jax.sharding import PartitionSpec as P


highest = lax.Precision.HIGHEST
f32 = jnp.float32
bf16 = jnp.bfloat16
LANES = 128
SUBLANES = 8
TILE = 16
AXES = ("pix", "row")


def contract_last(a, b):
    return lax.dot_general(a, b, (((1,), (1,)), ((), ())), preferred_element_type=f32)


def hot(shape, test):
    row = lax.broadcasted_iota(jnp.int32, shape, 0)
    column = lax.broadcasted_iota(jnp.int32, shape, 1)
    return test(row, column).astype(f32).astype(bf16)


def swap_rows(outer, inner):
    size = outer * inner
    return hot((size, size), lambda m, r: r == (m % outer) * inner + m // outer)


def pick(band_images, pivots):
    band_dev, line_dev, cols = band_images.shape
    panels, panel = pivots.shape
    pivot_count = panels * panel
    taken = LANES // band_dev
    groups = line_dev // taken
    shift = cols.bit_length() - 1
    chunks = band_dev // TILE
    rows = TILE * line_dev
    wide = TILE * TILE

    def kernel(x_ref, far_ref, rows_ref, spec_ref, plan_ref, held_ref, piv_ref, sems):
        def copy(i):
            part = pl.ds(i * TILE, TILE)
            return pltpu.make_async_copy(x_ref.at[part], held_ref.at[part], sems.at[i])

        indices = pltpu.make_async_copy(far_ref, piv_ref, sems.at[chunks])
        indices.start()
        for i in range(chunks):
            copy(i).start()
        mixed = swap_rows(TILE, TILE)
        plan_ref[:wide] = mixed
        plan_ref[wide : 2 * wide] = hot((wide, wide), lambda m, r: m == r)
        tall = groups * TILE
        plan_ref[2 * wide :] = hot(
            (wide, wide), lambda m, r: r == (m // tall) * tall + (m % groups) * TILE + (m % tall) // groups
        )
        indices.wait()
        flat = jnp.concatenate([piv_ref[i : i + 1, :] for i in range(panels)], axis=1).astype(f32)
        own = lax.broadcasted_iota(jnp.int32, (pivot_count, pivot_count), 0) == lax.broadcasted_iota(
            jnp.int32, (pivot_count, pivot_count), 1
        )
        flat = jnp.sum(jnp.where(own, flat, 0.0), axis=1, keepdims=True).astype(jnp.int32)
        column = flat & (cols - 1)
        inner = (flat >> shift) - lax.axis_index("row").astype(jnp.int32) * line_dev
        chosen = hot((pivot_count, cols), lambda k, c: c == column)
        lane = lax.broadcasted_iota(jnp.int32, (pivot_count, rows), 1)
        inside = lane % line_dev == inner
        fold = hot((TILE, rows), lambda b, r: r // line_dev == b)
        for i in range(chunks):
            copy(i).wait()
            bands = slice(i * TILE, (i + 1) * TILE)
            found = contract_last(chosen, held_ref[bands].reshape(rows, cols))
            found = jnp.where(inside, found, 0.0).astype(bf16)
            spec_ref[bands, :] = contract_last(fold, found).astype(bf16)
            for h in range(line_dev // TILE):
                block = held_ref[bands, h * TILE : (h + 1) * TILE, :].reshape(wide, cols)
                block = jnp.dot(mixed, block, preferred_element_type=f32).astype(bf16)
                for k in range(TILE):
                    line = h * TILE + k
                    start = ((line % groups) * taken + line // groups) * band_dev + i * TILE
                    rows_ref[start : start + TILE, :] = block[k * TILE : (k + 1) * TILE]

    return pl.pallas_call(
        kernel,
        out_shape=(
            pltpu.VMEM((line_dev * band_dev, cols), bf16),
            pltpu.VMEM((band_dev, pivot_count), bf16),
            pltpu.VMEM((3 * wide, wide), bf16),
        ),
        in_specs=[pl.BlockSpec(memory_space=pl.ANY), pl.BlockSpec(memory_space=pl.ANY)],
        scratch_shapes=[
            pltpu.VMEM(band_images.shape, bf16),
            pltpu.VMEM(pivots.shape, pivots.dtype),
            pltpu.SemaphoreType.DMA((chunks + 1,)),
        ],
        name="pick",
    )(band_images, pivots)


def near(*arrays):
    return [pltpu.with_memory_space_constraint(v, pltpu.VMEM) for v in arrays]


def pack(ordered, plans):
    rows, cols = ordered.shape
    wide = plans.shape[1]
    sides = cols // wide

    def kernel(x_ref, plan_ref, out_ref, out_buf, sems):
        def give(j, q):
            part = (pl.ds(j * wide, wide), pl.ds(q * wide, wide))
            return pltpu.make_async_copy(out_buf.at[part], out_ref.at[part], sems.at[j, q])

        for j in range(sides):
            for q in range(rows // wide):
                side = slice(j * wide, (j + 1) * wide)
                part = slice(q * wide, (q + 1) * wide)
                out_buf[side, part] = contract_last(plan_ref[wide : 2 * wide], x_ref[part, side]).astype(bf16)
                give(j, q).start()
        for j in range(sides):
            for q in range(rows // wide):
                give(j, q).wait()

    return pl.pallas_call(
        kernel,
        out_shape=jax.ShapeDtypeStruct((cols, rows), bf16),
        out_specs=pl.BlockSpec(memory_space=pl.ANY),
        scratch_shapes=[
            pltpu.VMEM((cols, rows), bf16),
            pltpu.SemaphoreType.DMA((sides, rows // wide)),
        ],
        name="pack",
    )(*near(ordered, plans))


def finish(arrived, keep, gains, plans, row_count, band_dev, line_dev):
    sources, narrow, _ = arrived.shape
    taken = LANES // band_dev
    groups = line_dev // taken
    lines = row_count * line_dev
    bands = sources // row_count * band_dev
    kept = gains.shape[0] // 2
    width = 4
    joined = bands // LANES
    pieces = narrow // width

    def swap(low, high, shift, mask):
        return (
            jnp.where(mask, low, pltpu.roll(high, shift, 1)),
            jnp.where(mask, pltpu.roll(low, LANES - shift, 1), high),
        )

    def kernel(a_ref, keep_ref, gain_ref, plan_ref, res_ref, coef_ref, x_ref, hold_ref, res_buf, coef_buf, sems):
        def give(i):
            at = pl.ds(i * width, width)
            return pltpu.make_async_copy(res_buf.at[at], res_ref.at[at], sems.at[i])

        last = pltpu.make_async_copy(coef_buf, coef_ref, sems.at[pieces])
        lane = lax.broadcasted_iota(jnp.int32, (groups, LANES), 1)
        size = plan_ref.shape[1]
        for r in range(row_count):
            for j in range(joined):
                sides = []
                for n in range(taken // 2):
                    tall = []
                    for s in range(2):
                        source = (j * taken + s * (taken // 2) + n) * row_count + r
                        tall += [a_ref[source, :, g * LANES : (g + 1) * LANES] for g in range(groups)]
                    sides.append(jnp.concatenate(tall, axis=0))
                turned = jnp.dot(
                    plan_ref[2 * size :], jnp.concatenate(sides, axis=1), preferred_element_type=f32
                )
                for c in range(narrow):
                    v = []
                    for i in range(taken):
                        s, n = i // (taken // 2), i % (taken // 2)
                        start = (s * narrow + c) * groups
                        v.append(turned[start : start + groups, n * LANES : (n + 1) * LANES])
                    step = taken // 2
                    while step >= 1:
                        shift = step * band_dev
                        mask = (lane // shift) % 2 == 0
                        w = list(v)
                        for i in range(taken):
                            if (i // step) % 2 == 0:
                                w[i], w[i + step] = swap(v[i], v[i + step], shift, mask)
                        v = w
                        step //= 2
                    row = c * lines + r * line_dev
                    x_ref[row : row + line_dev, j * LANES : (j + 1) * LANES] = (
                        jnp.concatenate(v, axis=0).astype(bf16)
                    )
        for c in range(0, narrow, 2):
            found = contract_last(gain_ref[...], x_ref[c * lines : (c + 2) * lines, :])
            found = (found[:kept] + found[kept:]).astype(bf16)
            hold_ref[c] = found[:, :lines]
            hold_ref[c + 1] = found[:, lines:]
        for k in range(0, kept, 2 * narrow):
            tall = [
                jnp.concatenate([hold_ref[c, q : q + narrow, :] for c in range(narrow)], axis=0)
                for q in (k, k + narrow)
            ]
            turned = jnp.dot(
                plan_ref[:size], jnp.concatenate(tall, axis=1), preferred_element_type=f32
            ).astype(bf16)
            coef_buf[k : k + narrow] = turned[:, :lines].reshape(narrow, narrow, lines)
            coef_buf[k + narrow : k + 2 * narrow] = turned[:, lines:].reshape(narrow, narrow, lines)
        last.start()
        for p in range(pieces):
            pixels = x_ref[p * width * lines : (p + 1) * width * lines, :]
            both = jnp.dot(pixels, keep_ref[:bands], preferred_element_type=f32)
            both = both + jnp.dot(pixels, keep_ref[bands:], preferred_element_type=f32)
            res_buf[p * width : (p + 1) * width] = both.astype(bf16).reshape(width, lines, bands)
            give(p).start()
        last.wait()
        for p in range(pieces):
            give(p).wait()

    return pl.pallas_call(
        kernel,
        out_shape=(
            jax.ShapeDtypeStruct((narrow, lines, bands), bf16),
            jax.ShapeDtypeStruct((kept, narrow, lines), bf16),
        ),
        out_specs=(pl.BlockSpec(memory_space=pl.ANY), pl.BlockSpec(memory_space=pl.ANY)),
        scratch_shapes=[
            pltpu.VMEM((narrow * lines, bands), bf16),
            pltpu.VMEM((narrow, kept, lines), bf16),
            pltpu.VMEM((narrow, lines, bands), bf16),
            pltpu.VMEM((kept, narrow, lines), bf16),
            pltpu.SemaphoreType.DMA((pieces + 1,)),
        ],
        name="finish",
    )(*near(arrived, keep, gains, plans))


def parts_of(a, count):
    out = []
    for _ in range(count):
        high = a.astype(bf16)
        out.append(high)
        a = a - high.astype(f32)
    return out


def factor(spectra, parts):
    bands, count = spectra.shape
    half = count // 2
    width = 2 * count

    def row_of(tile, i):
        return jnp.broadcast_to(tile[i : i + 1, :], tile.shape)

    def lane_of(tile, i):
        return jnp.broadcast_to(tile[:, i : i + 1], tile.shape)

    def inverse_of(gram):
        row = lax.broadcasted_iota(jnp.int32, (count, count), 0)
        lane = lax.broadcasted_iota(jnp.int32, (count, count), 1)
        both = jnp.concatenate([gram, jnp.where(lane == row, 1.0, 0.0)], axis=1)
        tiles = [both[i : i + SUBLANES] for i in range(0, count, SUBLANES)]
        place = lax.broadcasted_iota(jnp.int32, (SUBLANES, width), 0)
        done = []
        for first in range(len(tiles)):
            live = range(first, len(tiles))
            columns = [
                {i: lane_of(tiles[i], first * SUBLANES + k) for i in live} for k in range(SUBLANES)
            ]
            kept = tiles[first]
            for k in range(SUBLANES):
                scale = lax.rsqrt(row_of(columns[k][first], k))
                column = {i: columns[k][i] * scale for i in live}
                top = row_of(tiles[first], k) * scale
                kept = jnp.where(place == k, top, kept)
                for q in range(k + 1, SUBLANES):
                    other = row_of(column[first], q)
                    for i in live:
                        columns[q][i] = columns[q][i] - column[i] * other
                for i in live:
                    tiles[i] = tiles[i] - column[i] * top
            done.append(kept)
        return jnp.concatenate(done, axis=0)[:, count:]

    def kernel(s_ref, keep_ref, gain_ref):
        me = lax.axis_index("pix").astype(jnp.int32)
        own = bands // parts
        s = jnp.concatenate(
            [s_ref[pl.ds(pl.multiple_of((me ^ k) * own, own), own), :] for k in range(parts)], axis=0
        )
        st = contract_last(hot((count, count), lambda k, q: k == q), s).astype(bf16)
        pieces = parts_of(inverse_of(contract_last(st, st)), 3)
        basis = sum(contract_last(p, s) for p in pieces[::-1])
        tall = sum(contract_last(s, p) for p in pieces[::-1])
        high, low = parts_of(basis, 2)
        one, two = slice(0, half), slice(half, count)

        def products(a, b):
            return contract_last(high[a], high[b]) + (contract_last(high[a], low[b]) + contract_last(low[a], high[b]))

        across = products(one, two)
        back = products(two, one)

        def times(a, b):
            a_high, a_low = parts_of(a, 2)
            b_high, b_low = parts_of(b, 2)
            return jnp.dot(
                jnp.concatenate([a_high, a_low, a_high], axis=1),
                jnp.concatenate([b_high, b_high, b_low], axis=0),
                preferred_element_type=f32,
            )

        gains = jnp.concatenate([basis[one], basis[two] - times(back, basis[one])], axis=0)
        other = jnp.concatenate([tall[:, one], tall[:, two] - times(tall[:, one], across)], axis=1)
        eye = jnp.where(
            lax.broadcasted_iota(jnp.int32, (bands, bands), 0)
            == lax.broadcasted_iota(jnp.int32, (bands, bands), 1),
            1.0,
            0.0,
        )
        keep = eye - times(other, basis)
        for ref, value, size in ((keep_ref, keep, bands), (gain_ref, gains, count)):
            ref[:size], ref[size:] = parts_of(value, 2)

    return pl.pallas_call(
        kernel,
        out_shape=(
            pltpu.VMEM((2 * bands, bands), bf16),
            pltpu.VMEM((2 * count, bands), bf16),
        ),
        name="factor",
    )(*near(spectra))


def exchange(x, axis, k):
    count = lax.axis_size(axis)
    return lax.ppermute(x, axis, [(i, i ^ k) for i in range(count)])


def orthonormal(spectra):
    gram = jnp.dot(spectra, spectra.T, precision=highest)
    factor = jnp.linalg.cholesky(gram)
    return jax.scipy.linalg.solve_triangular(factor, spectra, lower=True)


def project(block, basis):
    count = basis.shape[0] // 2
    first = basis[:count]
    second = basis[count:]
    coef_one = jnp.einsum("clb,kb->kcl", block, first, precision=highest)
    remain = block - jnp.einsum("kcl,kb->clb", coef_one, first, precision=highest)
    coef_two = jnp.einsum("clb,kb->kcl", remain, second, precision=highest)
    remain = remain - jnp.einsum("kcl,kb->clb", coef_two, second, precision=highest)
    return (
        remain.astype(bf16),
        jnp.concatenate([coef_one, coef_two], axis=0).astype(bf16),
    )


def plain(band_images, line_index, column, pix_count, row_count, narrow):
    band_dev, line_dev, cols_all = band_images.shape
    offset = line_index - lax.axis_index("row") * line_dev
    inside = (offset >= 0) & (offset < line_dev)
    position = jnp.clip(offset, 0, line_dev - 1) * cols_all + column
    picked = jnp.take(band_images.reshape(band_dev, line_dev * cols_all), position, axis=1)
    picked = jnp.where(inside[None, :], picked, jnp.zeros_like(picked))
    stacked = lax.all_gather(picked, "pix", axis=0, tiled=True)
    spectra = lax.psum(stacked.astype(f32).astype(bf16), "row").astype(f32)
    basis = orthonormal(spectra.T)
    shaped = band_images.reshape(band_dev, line_dev, pix_count, row_count, narrow)
    arrived = lax.all_to_all(
        lax.all_to_all(shaped, "pix", split_axis=2, concat_axis=0, tiled=True),
        "row",
        split_axis=3,
        concat_axis=1,
        tiled=True,
    )
    block = (
        arrived.reshape(arrived.shape[0], arrived.shape[1], narrow)
        .transpose(2, 1, 0)
        .astype(f32)
    )
    return project(block, basis)


def shards(band_images, pivots):
    band_dev, line_dev, cols_all = band_images.shape
    pix_count = lax.axis_size("pix")
    row_count = lax.axis_size("row")
    part_count = pix_count * row_count
    narrow = cols_all // part_count
    flat_pivots = pivots.reshape(-1)
    pivot_count = flat_pivots.shape[0]
    line_index = flat_pivots // cols_all
    column = flat_pivots % cols_all
    lines = row_count * line_dev
    bands = pix_count * band_dev
    taken = LANES // band_dev
    fits = (
        taken in (2, 4)
        and taken * band_dev == LANES
        and line_dev == SUBLANES * taken
        and band_dev % TILE == 0
        and line_dev % TILE == 0
        and narrow == TILE
        and lines == LANES
        and bands % LANES == 0
        and 2 * pivot_count == LANES
        and cols_all % (TILE * TILE) == 0
        and cols_all & (cols_all - 1) == 0
        and pix_count & (pix_count - 1) == 0
        and row_count & (row_count - 1) == 0
    )
    if not fits:
        return plain(band_images, line_index, column, pix_count, row_count, narrow)
    ordered, picked, plans = pick(band_images, pivots)
    found = picked
    for k in range(row_count.bit_length() - 2, 0, -1):
        found = found + exchange(found, "row", 1 << k)
    packed = pack(ordered, plans).reshape(part_count, narrow, line_dev * band_dev)
    arrived = lax.all_to_all(packed, AXES, 0, 0, tiled=True)
    for k in range(pix_count.bit_length() - 1):
        found = jnp.concatenate([found, exchange(found, "pix", 1 << k)], axis=0)
    found = found + exchange(found, "row", 1)
    keep, gains = factor(found, pix_count)
    return finish(arrived, keep, gains, plans, row_count, band_dev, line_dev)


def solution(mesh):
    placed = (P("pix", "row", None), P())
    return jax.shard_map(
        shards,
        mesh=mesh,
        in_specs=placed,
        out_specs=(P(AXES, None, None), P(None, AXES, None)),
        check_vma=False,
    )
```

```python
import jax
import jax.numpy as jnp
from jax import lax
from jax.experimental import pallas as pl
from jax.experimental.pallas import tpu as pltpu
from jax.sharding import PartitionSpec as P


highest = lax.Precision.HIGHEST
f32 = jnp.float32
bf16 = jnp.bfloat16
LANES = 128
SUBLANES = 8
TILE = 16
AXES = ("pix", "row")


def contract_last(a, b):
    return lax.dot_general(a, b, (((1,), (1,)), ((), ())), preferred_element_type=f32)


def hot(shape, test):
    row = lax.broadcasted_iota(jnp.int32, shape, 0)
    column = lax.broadcasted_iota(jnp.int32, shape, 1)
    return test(row, column).astype(f32).astype(bf16)


def swap_rows(outer, inner):
    size = outer * inner
    return hot((size, size), lambda m, r: r == (m % outer) * inner + m // outer)


def pack(band_images, pivots):
    band_dev, line_dev, cols = band_images.shape
    panels, panel = pivots.shape
    pivot_count = panels * panel
    taken = LANES // band_dev
    groups = line_dev // taken
    shift = cols.bit_length() - 1
    chunks = band_dev // TILE
    rows = TILE * line_dev
    every = band_dev * line_dev
    wide = TILE * TILE
    sides = cols // wide

    def kernel(x_ref, far_ref, out_ref, spec_ref, plan_ref, held_ref, piv_ref, rows_ref, out_buf, sems, out_sems):
        def copy(i):
            part = pl.ds(i * TILE, TILE)
            return pltpu.make_async_copy(x_ref.at[part], held_ref.at[part], sems.at[i])

        def give(j, q):
            part = (pl.ds(j * wide, wide), pl.ds(q * wide, wide))
            return pltpu.make_async_copy(out_buf.at[part], out_ref.at[part], out_sems.at[j, q])

        indices = pltpu.make_async_copy(far_ref, piv_ref, sems.at[chunks])
        indices.start()
        for i in range(chunks):
            copy(i).start()
        mixed = swap_rows(TILE, TILE)
        plan_ref[:wide] = mixed
        plan_ref[wide : 2 * wide] = hot((wide, wide), lambda m, r: m == r)
        tall = groups * TILE
        plan_ref[2 * wide :] = hot(
            (wide, wide), lambda m, r: r == (m // tall) * tall + (m % groups) * TILE + (m % tall) // groups
        )
        indices.wait()
        flat = jnp.concatenate([piv_ref[i : i + 1, :] for i in range(panels)], axis=1).astype(f32)
        own = lax.broadcasted_iota(jnp.int32, (pivot_count, pivot_count), 0) == lax.broadcasted_iota(
            jnp.int32, (pivot_count, pivot_count), 1
        )
        flat = jnp.sum(jnp.where(own, flat, 0.0), axis=1, keepdims=True).astype(jnp.int32)
        column = flat & (cols - 1)
        inner = (flat >> shift) - lax.axis_index("row").astype(jnp.int32) * line_dev
        chosen = hot((pivot_count, cols), lambda k, c: c == column)
        lane = lax.broadcasted_iota(jnp.int32, (pivot_count, rows), 1)
        inside = lane % line_dev == inner
        fold = hot((TILE, rows), lambda b, r: r // line_dev == b)

        def find(i):
            bands = slice(i * TILE, (i + 1) * TILE)
            found = contract_last(chosen, held_ref[bands].reshape(rows, cols))
            found = jnp.where(inside, found, 0.0).astype(bf16)
            spec_ref[bands, :] = contract_last(fold, found).astype(bf16)

        for i in range(chunks):
            copy(i).wait()
            bands = slice(i * TILE, (i + 1) * TILE)
            for side in range(0, cols, wide):
                for h in range(line_dev // TILE):
                    block = held_ref[bands, h * TILE : (h + 1) * TILE, side : side + wide].reshape(wide, wide)
                    block = jnp.dot(mixed, block, preferred_element_type=f32).astype(bf16)
                    for k in range(TILE):
                        line = h * TILE + k
                        start = ((line % groups) * taken + line // groups) * band_dev + i * TILE
                        rows_ref[start : start + TILE, side : side + wide] = block[k * TILE : (k + 1) * TILE]
            find(i)
        for j in range(sides):
            for q in range(every // wide):
                side = slice(j * wide, (j + 1) * wide)
                part = slice(q * wide, (q + 1) * wide)
                out_buf[side, part] = contract_last(plan_ref[wide : 2 * wide], rows_ref[part, side]).astype(bf16)
                give(j, q).start()
        for j in range(sides):
            for q in range(every // wide):
                give(j, q).wait()

    return pl.pallas_call(
        kernel,
        out_shape=(
            jax.ShapeDtypeStruct((cols, every), bf16),
            pltpu.VMEM((band_dev, pivot_count), bf16),
            pltpu.VMEM((3 * wide, wide), bf16),
        ),
        in_specs=[pl.BlockSpec(memory_space=pl.ANY), pl.BlockSpec(memory_space=pl.ANY)],
        out_specs=(
            pl.BlockSpec(memory_space=pl.ANY),
            pl.BlockSpec(memory_space=pltpu.VMEM),
            pl.BlockSpec(memory_space=pltpu.VMEM),
        ),
        scratch_shapes=[
            pltpu.VMEM(band_images.shape, bf16),
            pltpu.VMEM(pivots.shape, pivots.dtype),
            pltpu.VMEM((every, cols), bf16),
            pltpu.VMEM((cols, every), bf16),
            pltpu.SemaphoreType.DMA((chunks + 1,)),
            pltpu.SemaphoreType.DMA((sides, every // wide)),
        ],
        name="pack",
    )(band_images, pivots)


def near(*arrays):
    return [pltpu.with_memory_space_constraint(v, pltpu.VMEM) for v in arrays]


def finish(arrived, keep, gains, plans, row_count, band_dev, line_dev):
    sources, narrow, _ = arrived.shape
    taken = LANES // band_dev
    groups = line_dev // taken
    lines = row_count * line_dev
    bands = sources // row_count * band_dev
    kept = gains.shape[0] // 2
    width = 4
    joined = bands // LANES
    pieces = narrow // width
    halves = 2

    def swap(low, high, shift, mask):
        return (
            jnp.where(mask, low, pltpu.roll(high, shift, 1)),
            jnp.where(mask, pltpu.roll(low, LANES - shift, 1), high),
        )

    def kernel(a_ref, keep_ref, gain_ref, plan_ref, res_ref, coef_ref, x_ref, hold_ref, res_buf, coef_buf, sems):
        def give(i):
            at = pl.ds(i * width, width)
            return pltpu.make_async_copy(res_buf.at[at], res_ref.at[at], sems.at[i])

        last = pltpu.make_async_copy(coef_buf, coef_ref, sems.at[pieces])
        lane = lax.broadcasted_iota(jnp.int32, (groups, LANES), 1)
        size = plan_ref.shape[1]

        def project(p):
            pixels = x_ref[p * width * lines : (p + 1) * width * lines, :]
            both = jnp.dot(jnp.concatenate([pixels, pixels], axis=1), keep_ref[...], preferred_element_type=f32)
            res_buf[p * width : (p + 1) * width] = both.astype(bf16).reshape(width, lines, bands)
            give(p).start()

        part = narrow // halves
        short = part * groups

        def gather(h, r, j):
            top = 2 * size + h * short
            mix = jnp.concatenate([plan_ref[top : top + short], plan_ref[top + size // 2 : top + size // 2 + short]], axis=0)
            sides = []
            for n in range(taken // 2):
                tall = []
                for s in range(2):
                    source = (j * taken + s * (taken // 2) + n) * row_count + r
                    tall += [a_ref[source, :, g * LANES : (g + 1) * LANES] for g in range(groups)]
                sides.append(jnp.concatenate(tall, axis=0))
            turned = jnp.dot(
                mix, jnp.concatenate(sides, axis=1), preferred_element_type=f32
            )
            for c in range(part):
                v = []
                for i in range(taken):
                    s, n = i // (taken // 2), i % (taken // 2)
                    start = (s * part + c) * groups
                    v.append(turned[start : start + groups, n * LANES : (n + 1) * LANES])
                step = taken // 2
                while step >= 1:
                    shift = step * band_dev
                    mask = (lane // shift) % 2 == 0
                    w = list(v)
                    for i in range(taken):
                        if (i // step) % 2 == 0:
                            w[i], w[i + step] = swap(v[i], v[i + step], shift, mask)
                    v = w
                    step //= 2
                row = (h * part + c) * lines + r * line_dev
                x_ref[row : row + line_dev, j * LANES : (j + 1) * LANES] = (
                    jnp.concatenate(v, axis=0).astype(bf16)
                )

        places = [(r, j) for r in range(row_count) for j in range(joined)]
        for h in range(halves):
            for i, (r, j) in enumerate(places):
                gather(h, r, j)
                if False and (i + 1) * (pieces // halves) % len(places) == 0:
                    project((h - 1) * (pieces // halves) + (i + 1) * (pieces // halves) // len(places) - 1)
        for p in range(pieces // 2):
            project(p)
        for c in range(0, narrow, 2):
            found = contract_last(gain_ref[...], x_ref[c * lines : (c + 2) * lines, :])
            found = (found[:kept] + found[kept:]).astype(bf16)
            hold_ref[c] = found[:, :lines]
            hold_ref[c + 1] = found[:, lines:]
        for k in range(0, kept, 2 * narrow):
            tall = [
                jnp.concatenate([hold_ref[c, q : q + narrow, :] for c in range(narrow)], axis=0)
                for q in (k, k + narrow)
            ]
            turned = jnp.dot(
                plan_ref[:size], jnp.concatenate(tall, axis=1), preferred_element_type=f32
            ).astype(bf16)
            coef_buf[k : k + narrow] = turned[:, :lines].reshape(narrow, narrow, lines)
            coef_buf[k + narrow : k + 2 * narrow] = turned[:, lines:].reshape(narrow, narrow, lines)
        last.start()
        for p in range(pieces // 2, pieces):
            project(p)
        last.wait()
        for p in range(pieces):
            give(p).wait()

    return pl.pallas_call(
        kernel,
        out_shape=(
            jax.ShapeDtypeStruct((narrow, lines, bands), bf16),
            jax.ShapeDtypeStruct((kept, narrow, lines), bf16),
        ),
        out_specs=(pl.BlockSpec(memory_space=pl.ANY), pl.BlockSpec(memory_space=pl.ANY)),
        scratch_shapes=[
            pltpu.VMEM((narrow * lines, bands), bf16),
            pltpu.VMEM((narrow, kept, lines), bf16),
            pltpu.VMEM((narrow, lines, bands), bf16),
            pltpu.VMEM((kept, narrow, lines), bf16),
            pltpu.SemaphoreType.DMA((pieces + 1,)),
        ],
        name="finish",
    )(*near(arrived, keep, gains, plans))


def parts_of(a, count):
    out = []
    for _ in range(count):
        high = a.astype(bf16)
        out.append(high)
        a = a - high.astype(f32)
    return out


def factor(spectra, parts):
    bands, count = spectra.shape
    half = count // 2
    width = 2 * count

    def row_of(tile, i):
        return jnp.broadcast_to(tile[i : i + 1, :], tile.shape)

    def lane_of(tile, i):
        return jnp.broadcast_to(tile[:, i : i + 1], tile.shape)

    def inverse_of(gram):
        row = lax.broadcasted_iota(jnp.int32, (count, count), 0)
        lane = lax.broadcasted_iota(jnp.int32, (count, count), 1)
        both = jnp.concatenate([gram, jnp.where(lane == row, 1.0, 0.0)], axis=1)
        tiles = [both[i : i + SUBLANES] for i in range(0, count, SUBLANES)]
        place = lax.broadcasted_iota(jnp.int32, (SUBLANES, width), 0)
        done = []
        for first in range(len(tiles)):
            live = range(first, len(tiles))
            columns = [
                {i: lane_of(tiles[i], first * SUBLANES + k) for i in live} for k in range(SUBLANES)
            ]
            kept = tiles[first]
            for k in range(SUBLANES):
                scale = lax.rsqrt(row_of(columns[k][first], k))
                column = {i: columns[k][i] * scale for i in live}
                top = row_of(tiles[first], k) * scale
                kept = jnp.where(place == k, top, kept)
                for q in range(k + 1, SUBLANES):
                    other = row_of(column[first], q)
                    for i in live:
                        columns[q][i] = columns[q][i] - column[i] * other
                for i in live:
                    tiles[i] = tiles[i] - column[i] * top
            done.append(kept)
        return jnp.concatenate(done, axis=0)[:, count:]

    def kernel(s_ref, keep_ref, gain_ref):
        me = lax.axis_index("pix").astype(jnp.int32)
        own = bands // parts
        s = jnp.concatenate(
            [s_ref[pl.ds(pl.multiple_of((me ^ k) * own, own), own), :] for k in range(parts)], axis=0
        )
        st = contract_last(hot((count, count), lambda k, q: k == q), s).astype(bf16)
        pieces = parts_of(inverse_of(contract_last(st, st)), 3)
        basis = sum(contract_last(p, s) for p in pieces[::-1])
        tall = sum(contract_last(s, p) for p in pieces[::-1])
        high, low = parts_of(basis, 2)
        one, two = slice(0, half), slice(half, count)

        def products(a, b):
            return contract_last(high[a], high[b]) + (contract_last(high[a], low[b]) + contract_last(low[a], high[b]))

        across = products(one, two)
        back = products(two, one)

        def times(a, b):
            a_high, a_low = parts_of(a, 2)
            b_high, b_low = parts_of(b, 2)
            return jnp.dot(
                jnp.concatenate([a_high, a_low, a_high], axis=1),
                jnp.concatenate([b_high, b_high, b_low], axis=0),
                preferred_element_type=f32,
            )

        gains = jnp.concatenate([basis[one], basis[two] - times(back, basis[one])], axis=0)
        other = jnp.concatenate([tall[:, one], tall[:, two] - times(tall[:, one], across)], axis=1)
        eye = jnp.where(
            lax.broadcasted_iota(jnp.int32, (bands, bands), 0)
            == lax.broadcasted_iota(jnp.int32, (bands, bands), 1),
            1.0,
            0.0,
        )
        keep = eye - times(other, basis)
        for ref, value, size in ((keep_ref, keep, bands), (gain_ref, gains, count)):
            ref[:size], ref[size:] = parts_of(value, 2)

    return pl.pallas_call(
        kernel,
        out_shape=(
            pltpu.VMEM((2 * bands, bands), bf16),
            pltpu.VMEM((2 * count, bands), bf16),
        ),
        name="factor",
    )(*near(spectra))


def exchange(x, axis, k):
    count = lax.axis_size(axis)
    return lax.ppermute(x, axis, [(i, i ^ k) for i in range(count)])


def orthonormal(spectra):
    gram = jnp.dot(spectra, spectra.T, precision=highest)
    factor = jnp.linalg.cholesky(gram)
    return jax.scipy.linalg.solve_triangular(factor, spectra, lower=True)


def project(block, basis):
    count = basis.shape[0] // 2
    first = basis[:count]
    second = basis[count:]
    coef_one = jnp.einsum("clb,kb->kcl", block, first, precision=highest)
    remain = block - jnp.einsum("kcl,kb->clb", coef_one, first, precision=highest)
    coef_two = jnp.einsum("clb,kb->kcl", remain, second, precision=highest)
    remain = remain - jnp.einsum("kcl,kb->clb", coef_two, second, precision=highest)
    return (
        remain.astype(bf16),
        jnp.concatenate([coef_one, coef_two], axis=0).astype(bf16),
    )


def plain(band_images, line_index, column, pix_count, row_count, narrow):
    band_dev, line_dev, cols_all = band_images.shape
    offset = line_index - lax.axis_index("row") * line_dev
    inside = (offset >= 0) & (offset < line_dev)
    position = jnp.clip(offset, 0, line_dev - 1) * cols_all + column
    picked = jnp.take(band_images.reshape(band_dev, line_dev * cols_all), position, axis=1)
    picked = jnp.where(inside[None, :], picked, jnp.zeros_like(picked))
    stacked = lax.all_gather(picked, "pix", axis=0, tiled=True)
    spectra = lax.psum(stacked.astype(f32).astype(bf16), "row").astype(f32)
    basis = orthonormal(spectra.T)
    shaped = band_images.reshape(band_dev, line_dev, pix_count, row_count, narrow)
    arrived = lax.all_to_all(
        lax.all_to_all(shaped, "pix", split_axis=2, concat_axis=0, tiled=True),
        "row",
        split_axis=3,
        concat_axis=1,
        tiled=True,
    )
    block = (
        arrived.reshape(arrived.shape[0], arrived.shape[1], narrow)
        .transpose(2, 1, 0)
        .astype(f32)
    )
    return project(block, basis)


def shards(band_images, pivots):
    band_dev, line_dev, cols_all = band_images.shape
    pix_count = lax.axis_size("pix")
    row_count = lax.axis_size("row")
    part_count = pix_count * row_count
    narrow = cols_all // part_count
    flat_pivots = pivots.reshape(-1)
    pivot_count = flat_pivots.shape[0]
    line_index = flat_pivots // cols_all
    column = flat_pivots % cols_all
    lines = row_count * line_dev
    bands = pix_count * band_dev
    taken = LANES // band_dev
    fits = (
        taken in (2, 4)
        and taken * band_dev == LANES
        and line_dev == SUBLANES * taken
        and band_dev % TILE == 0
        and line_dev % TILE == 0
        and narrow == TILE
        and lines == LANES
        and bands % LANES == 0
        and 2 * pivot_count == LANES
        and cols_all % (TILE * TILE) == 0
        and cols_all & (cols_all - 1) == 0
        and pix_count & (pix_count - 1) == 0
        and row_count & (row_count - 1) == 0
    )
    if not fits:
        return plain(band_images, line_index, column, pix_count, row_count, narrow)
    packed, found, plans = pack(band_images, pivots)
    packed = packed.reshape(part_count, narrow, line_dev * band_dev)
    for k in range(row_count.bit_length() - 2, 0, -1):
        found = found + exchange(found, "row", 1 << k)
    arrived = lax.all_to_all(packed, AXES, 0, 0, tiled=True)
    for k in range(pix_count.bit_length() - 1):
        found = jnp.concatenate([found, exchange(found, "pix", 1 << k)], axis=0)
    found = found + exchange(found, "row", 1)
    keep, gains = factor(found, pix_count)
    return finish(arrived, keep, gains, plans, row_count, band_dev, line_dev)


def solution(mesh):
    placed = (P("pix", "row", None), P())
    return jax.shard_map(
        shards,
        mesh=mesh,
        in_specs=placed,
        out_specs=(P(AXES, None, None), P(None, AXES, None)),
        check_vma=False,
    )
```

```python
import jax
import jax.numpy as jnp
from jax import lax
from jax.experimental import pallas as pl
from jax.experimental.pallas import tpu as pltpu
from jax.sharding import PartitionSpec as P


highest = lax.Precision.HIGHEST
f32 = jnp.float32
bf16 = jnp.bfloat16
LANES = 128
SUBLANES = 8
TILE = 16
AXES = ("pix", "row")


def contract_last(a, b):
    return lax.dot_general(a, b, (((1,), (1,)), ((), ())), preferred_element_type=f32)


def hot(shape, test):
    row = lax.broadcasted_iota(jnp.int32, shape, 0)
    column = lax.broadcasted_iota(jnp.int32, shape, 1)
    return test(row, column).astype(f32).astype(bf16)


def swap_rows(outer, inner):
    size = outer * inner
    return hot((size, size), lambda m, r: r == (m % outer) * inner + m // outer)


def pack(band_images, pivots):
    band_dev, line_dev, cols = band_images.shape
    panels, panel = pivots.shape
    pivot_count = panels * panel
    taken = LANES // band_dev
    groups = line_dev // taken
    shift = cols.bit_length() - 1
    chunks = band_dev // TILE
    rows = TILE * line_dev
    every = band_dev * line_dev
    wide = TILE * TILE
    sides = cols // wide

    def kernel(x_ref, far_ref, out_ref, spec_ref, plan_ref, held_ref, piv_ref, rows_ref, out_buf, sems, out_sems):
        def copy(i):
            part = (slice(None), slice(None), pl.ds(i * wide, wide))
            return pltpu.make_async_copy(x_ref.at[part], held_ref.at[part], sems.at[i])

        def give(j, q):
            part = (pl.ds(j * wide, wide), pl.ds(q * wide, wide))
            return pltpu.make_async_copy(out_buf.at[part], out_ref.at[part], out_sems.at[j, q])

        indices = pltpu.make_async_copy(far_ref, piv_ref, sems.at[sides])
        indices.start()
        for i in range(sides):
            copy(i).start()
        mixed = swap_rows(TILE, TILE)
        plan_ref[:wide] = mixed
        plan_ref[wide : 2 * wide] = hot((wide, wide), lambda m, r: m == r)
        tall = groups * TILE
        plan_ref[2 * wide :] = hot(
            (wide, wide), lambda m, r: r == (m // tall) * tall + (m % groups) * TILE + (m % tall) // groups
        )
        indices.wait()
        flat = jnp.concatenate([piv_ref[i : i + 1, :] for i in range(panels)], axis=1).astype(f32)
        own = lax.broadcasted_iota(jnp.int32, (pivot_count, pivot_count), 0) == lax.broadcasted_iota(
            jnp.int32, (pivot_count, pivot_count), 1
        )
        flat = jnp.sum(jnp.where(own, flat, 0.0), axis=1, keepdims=True).astype(jnp.int32)
        column = flat & (cols - 1)
        inner = (flat >> shift) - lax.axis_index("row").astype(jnp.int32) * line_dev
        chosen = hot((pivot_count, cols), lambda k, c: c == column)
        lane = lax.broadcasted_iota(jnp.int32, (pivot_count, rows), 1)
        inside = lane % line_dev == inner
        fold = hot((TILE, rows), lambda b, r: r // line_dev == b)

        def turn(j, i, h):
            side = slice(j * wide, (j + 1) * wide)
            block = held_ref[i * TILE : (i + 1) * TILE, h * TILE : (h + 1) * TILE, side].reshape(wide, wide)
            block = jnp.dot(mixed, block, preferred_element_type=f32).astype(bf16)
            for k in range(TILE):
                line = h * TILE + k
                start = ((line % groups) * taken + line // groups) * band_dev + i * TILE
                rows_ref[start : start + TILE, side] = block[k * TILE : (k + 1) * TILE]

        def find(i):
            bands = slice(i * TILE, (i + 1) * TILE)
            found = contract_last(chosen, held_ref[bands].reshape(rows, cols))
            found = jnp.where(inside, found, 0.0).astype(bf16)
            spec_ref[bands, :] = contract_last(fold, found).astype(bf16)

        def send(j, q):
            side = slice(j * wide, (j + 1) * wide)
            part = slice(q * wide, (q + 1) * wide)
            out_buf[side, part] = contract_last(plan_ref[wide : 2 * wide], rows_ref[part, side]).astype(bf16)
            give(j, q).start()

        blocks = [(i, h) for i in range(chunks) for h in range(line_dev // TILE)]
        parts = range(every // wide)
        for j in range(sides):
            copy(j).wait()
            for i, h in blocks:
                turn(j, i, h)
            if j > 0:
                for q in parts:
                    send(j - 1, q)
        for i in range(chunks):
            find(i)
        for q in parts:
            send(sides - 1, q)
        for j in range(sides):
            for q in range(every // wide):
                give(j, q).wait()

    return pl.pallas_call(
        kernel,
        out_shape=(
            jax.ShapeDtypeStruct((cols, every), bf16),
            pltpu.VMEM((band_dev, pivot_count), bf16),
            pltpu.VMEM((3 * wide, wide), bf16),
        ),
        in_specs=[pl.BlockSpec(memory_space=pl.ANY), pl.BlockSpec(memory_space=pl.ANY)],
        out_specs=(
            pl.BlockSpec(memory_space=pl.ANY),
            pl.BlockSpec(memory_space=pltpu.VMEM),
            pl.BlockSpec(memory_space=pltpu.VMEM),
        ),
        scratch_shapes=[
            pltpu.VMEM(band_images.shape, bf16),
            pltpu.VMEM(pivots.shape, pivots.dtype),
            pltpu.VMEM((every, cols), bf16),
            pltpu.VMEM((cols, every), bf16),
            pltpu.SemaphoreType.DMA((sides + 1,)),
            pltpu.SemaphoreType.DMA((sides, every // wide)),
        ],
        name="pack",
    )(band_images, pivots)


def near(*arrays):
    return [pltpu.with_memory_space_constraint(v, pltpu.VMEM) for v in arrays]


def finish(arrived, keep, gains, plans, row_count, band_dev, line_dev):
    sources, narrow, _ = arrived.shape
    taken = LANES // band_dev
    groups = line_dev // taken
    lines = row_count * line_dev
    bands = sources // row_count * band_dev
    kept = gains.shape[0] // 2
    width = 4
    joined = bands // LANES
    halves = 1
    steps = [(c, width) for c in range(0, narrow, width)]
    pieces = len(steps)
    early = 2

    def swap(low, high, shift, mask):
        return (
            jnp.where(mask, low, pltpu.roll(high, shift, 1)),
            jnp.where(mask, pltpu.roll(low, LANES - shift, 1), high),
        )

    def kernel(a_ref, keep_ref, gain_ref, plan_ref, res_ref, coef_ref, x_ref, hold_ref, res_buf, coef_buf, sems):
        def give(i):
            at = pl.ds(*steps[i])
            return pltpu.make_async_copy(res_buf.at[at], res_ref.at[at], sems.at[i])

        last = pltpu.make_async_copy(coef_buf, coef_ref, sems.at[pieces])
        lane = lax.broadcasted_iota(jnp.int32, (groups, LANES), 1)
        size = plan_ref.shape[1]

        def project(p):
            first, count = steps[p]
            pixels = x_ref[first * lines : (first + count) * lines, :]
            both = jnp.dot(jnp.concatenate([pixels, pixels], axis=1), keep_ref[...], preferred_element_type=f32)
            res_buf[first : first + count] = both.astype(bf16).reshape(count, lines, bands)
            give(p).start()

        part = narrow // halves
        short = part * groups

        def gather(h, r, j):
            top = 2 * size + h * short
            mix = jnp.concatenate([plan_ref[top : top + short], plan_ref[top + size // 2 : top + size // 2 + short]], axis=0)
            sides = []
            for n in range(taken // 2):
                tall = []
                for s in range(2):
                    source = (j * taken + s * (taken // 2) + n) * row_count + r
                    tall += [a_ref[source, :, g * LANES : (g + 1) * LANES] for g in range(groups)]
                sides.append(jnp.concatenate(tall, axis=0))
            turned = jnp.dot(
                mix, jnp.concatenate(sides, axis=1), preferred_element_type=f32
            )
            for c in range(part):
                v = []
                for i in range(taken):
                    s, n = i // (taken // 2), i % (taken // 2)
                    start = (s * part + c) * groups
                    v.append(turned[start : start + groups, n * LANES : (n + 1) * LANES])
                step = taken // 2
                while step >= 1:
                    shift = step * band_dev
                    mask = (lane // shift) % 2 == 0
                    w = list(v)
                    for i in range(taken):
                        if (i // step) % 2 == 0:
                            w[i], w[i + step] = swap(v[i], v[i + step], shift, mask)
                    v = w
                    step //= 2
                row = (h * part + c) * lines + r * line_dev
                x_ref[row : row + line_dev, j * LANES : (j + 1) * LANES] = (
                    jnp.concatenate(v, axis=0).astype(bf16)
                )

        places = [(r, j) for r in range(row_count) for j in range(joined)]
        for h in range(halves):
            for r, j in places:
                gather(h, r, j)
        for p in range(early):
            project(p)
        for c in range(0, narrow, 2):
            found = contract_last(gain_ref[...], x_ref[c * lines : (c + 2) * lines, :])
            found = (found[:kept] + found[kept:]).astype(bf16)
            hold_ref[c] = found[:, :lines]
            hold_ref[c + 1] = found[:, lines:]
        for k in range(0, kept, 2 * narrow):
            tall = [
                jnp.concatenate([hold_ref[c, q : q + narrow, :] for c in range(narrow)], axis=0)
                for q in (k, k + narrow)
            ]
            turned = jnp.dot(
                plan_ref[:size], jnp.concatenate(tall, axis=1), preferred_element_type=f32
            ).astype(bf16)
            coef_buf[k : k + narrow] = turned[:, :lines].reshape(narrow, narrow, lines)
            coef_buf[k + narrow : k + 2 * narrow] = turned[:, lines:].reshape(narrow, narrow, lines)
        last.start()
        for p in range(early, pieces):
            project(p)
        last.wait()
        for p in range(pieces):
            give(p).wait()

    return pl.pallas_call(
        kernel,
        out_shape=(
            jax.ShapeDtypeStruct((narrow, lines, bands), bf16),
            jax.ShapeDtypeStruct((kept, narrow, lines), bf16),
        ),
        out_specs=(pl.BlockSpec(memory_space=pl.ANY), pl.BlockSpec(memory_space=pl.ANY)),
        scratch_shapes=[
            pltpu.VMEM((narrow * lines, bands), bf16),
            pltpu.VMEM((narrow, kept, lines), bf16),
            pltpu.VMEM((narrow, lines, bands), bf16),
            pltpu.VMEM((kept, narrow, lines), bf16),
            pltpu.SemaphoreType.DMA((pieces + 1,)),
        ],
        name="finish",
    )(*near(arrived, keep, gains, plans))


def parts_of(a, count):
    out = []
    for _ in range(count):
        high = a.astype(bf16)
        out.append(high)
        a = a - high.astype(f32)
    return out


def factor(spectra, parts):
    bands, count = spectra.shape
    half = count // 2
    width = 2 * count

    def row_of(tile, i):
        return jnp.broadcast_to(tile[i : i + 1, :], tile.shape)

    def lane_of(tile, i):
        return jnp.broadcast_to(tile[:, i : i + 1], tile.shape)

    def inverse_of(gram):
        row = lax.broadcasted_iota(jnp.int32, (count, count), 0)
        lane = lax.broadcasted_iota(jnp.int32, (count, count), 1)
        both = jnp.concatenate([gram, jnp.where(lane == row, 1.0, 0.0)], axis=1)
        tiles = [both[i : i + SUBLANES] for i in range(0, count, SUBLANES)]
        place = lax.broadcasted_iota(jnp.int32, (SUBLANES, width), 0)
        done = []
        for first in range(len(tiles)):
            live = range(first, len(tiles))
            columns = [
                {i: lane_of(tiles[i], first * SUBLANES + k) for i in live} for k in range(SUBLANES)
            ]
            kept = tiles[first]
            for k in range(SUBLANES):
                scale = lax.rsqrt(row_of(columns[k][first], k))
                column = {i: columns[k][i] * scale for i in live}
                top = row_of(tiles[first], k) * scale
                kept = jnp.where(place == k, top, kept)
                for q in range(k + 1, SUBLANES):
                    other = row_of(column[first], q)
                    for i in live:
                        columns[q][i] = columns[q][i] - column[i] * other
                for i in live:
                    tiles[i] = tiles[i] - column[i] * top
            done.append(kept)
        return jnp.concatenate(done, axis=0)[:, count:]

    def kernel(s_ref, keep_ref, gain_ref):
        me = lax.axis_index("pix").astype(jnp.int32)
        own = bands // parts
        s = jnp.concatenate(
            [s_ref[pl.ds(pl.multiple_of((me ^ k) * own, own), own), :] for k in range(parts)], axis=0
        )
        st = contract_last(hot((count, count), lambda k, q: k == q), s).astype(bf16)
        pieces = parts_of(inverse_of(contract_last(st, st)), 3)
        basis = sum(contract_last(p, s) for p in pieces[::-1])
        tall = sum(contract_last(s, p) for p in pieces[::-1])
        high, low = parts_of(basis, 2)
        one, two = slice(0, half), slice(half, count)

        def products(a, b):
            return contract_last(high[a], high[b]) + (contract_last(high[a], low[b]) + contract_last(low[a], high[b]))

        across = products(one, two)
        back = products(two, one)

        def times(a, b):
            a_high, a_low = parts_of(a, 2)
            b_high, b_low = parts_of(b, 2)
            return jnp.dot(
                jnp.concatenate([a_high, a_low, a_high], axis=1),
                jnp.concatenate([b_high, b_high, b_low], axis=0),
                preferred_element_type=f32,
            )

        gains = jnp.concatenate([basis[one], basis[two] - times(back, basis[one])], axis=0)
        other = jnp.concatenate([tall[:, one], tall[:, two] - times(tall[:, one], across)], axis=1)
        eye = jnp.where(
            lax.broadcasted_iota(jnp.int32, (bands, bands), 0)
            == lax.broadcasted_iota(jnp.int32, (bands, bands), 1),
            1.0,
            0.0,
        )
        keep = eye - times(other, basis)
        for ref, value, size in ((keep_ref, keep, bands), (gain_ref, gains, count)):
            ref[:size], ref[size:] = parts_of(value, 2)

    return pl.pallas_call(
        kernel,
        out_shape=(
            pltpu.VMEM((2 * bands, bands), bf16),
            pltpu.VMEM((2 * count, bands), bf16),
        ),
        name="factor",
    )(*near(spectra))


def exchange(x, axis, k):
    count = lax.axis_size(axis)
    return lax.ppermute(x, axis, [(i, i ^ k) for i in range(count)])


def orthonormal(spectra):
    gram = jnp.dot(spectra, spectra.T, precision=highest)
    factor = jnp.linalg.cholesky(gram)
    return jax.scipy.linalg.solve_triangular(factor, spectra, lower=True)


def project(block, basis):
    count = basis.shape[0] // 2
    first = basis[:count]
    second = basis[count:]
    coef_one = jnp.einsum("clb,kb->kcl", block, first, precision=highest)
    remain = block - jnp.einsum("kcl,kb->clb", coef_one, first, precision=highest)
    coef_two = jnp.einsum("clb,kb->kcl", remain, second, precision=highest)
    remain = remain - jnp.einsum("kcl,kb->clb", coef_two, second, precision=highest)
    return (
        remain.astype(bf16),
        jnp.concatenate([coef_one, coef_two], axis=0).astype(bf16),
    )


def plain(band_images, line_index, column, pix_count, row_count, narrow):
    band_dev, line_dev, cols_all = band_images.shape
    offset = line_index - lax.axis_index("row") * line_dev
    inside = (offset >= 0) & (offset < line_dev)
    position = jnp.clip(offset, 0, line_dev - 1) * cols_all + column
    picked = jnp.take(band_images.reshape(band_dev, line_dev * cols_all), position, axis=1)
    picked = jnp.where(inside[None, :], picked, jnp.zeros_like(picked))
    stacked = lax.all_gather(picked, "pix", axis=0, tiled=True)
    spectra = lax.psum(stacked.astype(f32).astype(bf16), "row").astype(f32)
    basis = orthonormal(spectra.T)
    shaped = band_images.reshape(band_dev, line_dev, pix_count, row_count, narrow)
    arrived = lax.all_to_all(
        lax.all_to_all(shaped, "pix", split_axis=2, concat_axis=0, tiled=True),
        "row",
        split_axis=3,
        concat_axis=1,
        tiled=True,
    )
    block = (
        arrived.reshape(arrived.shape[0], arrived.shape[1], narrow)
        .transpose(2, 1, 0)
        .astype(f32)
    )
    return project(block, basis)


def shards(band_images, pivots):
    band_dev, line_dev, cols_all = band_images.shape
    pix_count = lax.axis_size("pix")
    row_count = lax.axis_size("row")
    part_count = pix_count * row_count
    narrow = cols_all // part_count
    flat_pivots = pivots.reshape(-1)
    pivot_count = flat_pivots.shape[0]
    line_index = flat_pivots // cols_all
    column = flat_pivots % cols_all
    lines = row_count * line_dev
    bands = pix_count * band_dev
    taken = LANES // band_dev
    fits = (
        taken in (2, 4)
        and taken * band_dev == LANES
        and line_dev == SUBLANES * taken
        and band_dev % TILE == 0
        and line_dev % TILE == 0
        and narrow == TILE
        and lines == LANES
        and bands % LANES == 0
        and 2 * pivot_count == LANES
        and cols_all % (TILE * TILE) == 0
        and cols_all & (cols_all - 1) == 0
        and pix_count & (pix_count - 1) == 0
        and row_count & (row_count - 1) == 0
    )
    if not fits:
        return plain(band_images, line_index, column, pix_count, row_count, narrow)
    packed, found, plans = pack(band_images, pivots)
    packed = packed.reshape(part_count, narrow, line_dev * band_dev)
    for k in range(row_count.bit_length() - 2, 0, -1):
        found = found + exchange(found, "row", 1 << k)
    arrived = lax.all_to_all(packed, AXES, 0, 0, tiled=True)
    for k in range(pix_count.bit_length() - 1):
        found = jnp.concatenate([found, exchange(found, "pix", 1 << k)], axis=0)
    found = found + exchange(found, "row", 1)
    keep, gains = factor(found, pix_count)
    return finish(arrived, keep, gains, plans, row_count, band_dev, line_dev)


def solution(mesh):
    placed = (P("pix", "row", None), P())
    return jax.shard_map(
        shards,
        mesh=mesh,
        in_specs=placed,
        out_specs=(P(AXES, None, None), P(None, AXES, None)),
        check_vma=False,
    )
```
